128 devices in a mesh: rep: 4 (over y_hi, core), grp: 32 (over y_lo, x, z).
Axes of the slice: x: 4, y: 4 (y_hi: 2, y_lo: 2; y = y_hi * 2 + y_lo), z: 4, core: 2. Of those that a mesh axis runs over, the one named last changes fastest.
Arguments:
- hidden_in: bfloat16 [512, 7168], P(('rep', 'grp')), may hold values from -3 to 3
- q_nope: bfloat16 [512, 8192], P(('rep', 'grp')), may hold values from -9 to 9
- q_rope: bfloat16 [512, 4096], P(('rep', 'grp')), may hold values from -36 to 36
- new_kv: bfloat16 [512, 576], P(('rep', 'grp')), may hold values from -6 to 6
- cache_kv: bfloat16 [512, 4096, 576], P(('rep', 'grp')), may hold values from -10 to 10
- lengths: int32 [512], P(('rep', 'grp')), may hold values from 2 to 4096, as said below
- w_uk: bfloat16 [512, 8192], P('rep'), may hold values from -0.5 to 0.5
- w_uv: bfloat16 [512, 8192], P('rep'), may hold values from -0.25 to 0.25
- w_out: bfloat16 [8192, 7168], P('grp'), may hold values from -0.0625 to 0.0625
- norm_gain: bfloat16 [7168], replicated, may hold values from 0.5 to 1.5
- w_gate: bfloat16 [7168, 18432], P(None, ('rep', 'grp')), may hold values from -0.0625 to 0.0625
- w_up: bfloat16 [7168, 18432], P(None, ('rep', 'grp')), may hold values from -0.0625 to 0.0625
- w_down: bfloat16 [18432, 7168], P(('rep', 'grp')), may hold values from -0.046875 to 0.046875
Outputs:
- hidden_out: bfloat16 [512, 7168], P(('rep', 'grp'))
The draws below stay inside these ranges and needn't reach their ends.
Inputs may be any that keep to these rules, and one draw needn't show every extreme that they name: `lengths`: every sequence has 2 or more cached positions and at most 4096; some sequence has exactly 4096.
All inputs are finite; a program needn't handle non-finite values.
Results may differ from the reference program's by a relative error of at most 0.03.
Values may be sent and summed in bfloat16 or wider, within the bound.
A program may use at most 192 MiB of HBM per device.

```python
import jax
import jax.numpy as jnp
from jax import lax

D = 7168
FF = 18432
H = 64
NOPE = 128
ROPE = 64
VH = 128
KV_RANK = 512
CACHE = 4096
SEQS = 512


def draw_q_rope(key, part):
    values = jnp.clip(jax.random.normal(jax.random.fold_in(key, 3), (SEQS, H, ROPE), jnp.float32), -6.0, 6.0)
    return values.reshape(SEQS, H * ROPE).astype(jnp.bfloat16)


def draw_cache_kv(key, part):
    inner = jax.random.fold_in(key, 4)
    values = jnp.clip(jax.random.normal(inner, (SEQS, CACHE, KV_RANK + ROPE), jnp.float32), -6.0, 6.0)
    return values.astype(jnp.bfloat16)


def draw_lengths(key, part):
    inner = jax.random.fold_in(key, 5)
    lengths_drawn = jax.random.randint(inner, (SEQS,), 2, CACHE + 1, dtype=jnp.int32)
    where_full = jax.random.randint(jax.random.fold_in(inner, 6), (), 0, SEQS, dtype=jnp.int32)
    return jnp.where(jnp.arange(SEQS, dtype=jnp.int32) == where_full, CACHE, lengths_drawn).astype(jnp.int32)


def block_levels(key, shape, split, smallest, high):
    def one(position, shards_of):
        steps = jax.random.uniform(jax.random.fold_in(jax.random.fold_in(key, 6), position), (shards_of,), jnp.float32, smallest / len(split), high / len(split))
        return jnp.repeat(jnp.exp(steps), shape[position] // shards_of).reshape((-1,) + (1,) * (len(shape) - position - 1))

    loudness = one(*split[0])
    for cut in split[1:]:
        loudness = loudness * one(*cut)
    return loudness


def normal_values(stream_key, extent, scale, bound, pieces=(), kind=jnp.bfloat16):
    array = jax.random.normal(stream_key, extent, jnp.float32) * scale
    if len(pieces) > 0:
        array = block_levels(stream_key, extent, pieces, -0.22, 0.18) * array
    return jnp.clip(array, min=-bound, max=bound).astype(kind)


def setup_inputs(seed: int = 0) -> dict:
    key_list = jax.random.split(jax.random.key(seed), 14)
    return {
        "hidden_in": normal_values(key_list[0], (SEQS, D), 0.5, 3.0, ((0, 128),)),
        "q_nope": normal_values(key_list[1], (SEQS, H * NOPE), 1.5, 9.0, ((0, 128),)),
        "q_rope": draw_q_rope(jax.random.fold_in(key_list[13], 71), 0),
        "new_kv": normal_values(key_list[3], (SEQS, KV_RANK + ROPE), 1.0, 6.0, ((0, 128),)),
        "cache_kv": draw_cache_kv(jax.random.fold_in(key_list[13], 71), 0),
        "lengths": draw_lengths(jax.random.fold_in(key_list[13], 71), 0),
        "w_uk": normal_values(key_list[6], (KV_RANK, H * NOPE), NOPE ** -0.5, 0.5, ((0, 4),)),
        "w_uv": normal_values(key_list[7], (KV_RANK, H * VH), KV_RANK ** -0.5, 0.25, ((0, 4),)),
        "w_out": normal_values(key_list[8], (H * VH, D), (H * VH) ** -0.5, 0.0625, ((0, 32),)),
        "norm_gain": jnp.clip(1.0 + 0.1 * jax.random.normal(key_list[9], (D,), jnp.float32), 0.5, 1.5).astype(jnp.bfloat16),
        "w_gate": normal_values(key_list[10], (D, FF), D ** -0.5, 0.0625, ((1, 128),)),
        "w_up": normal_values(key_list[11], (D, FF), D ** -0.5, 0.0625, ((1, 128),)),
        "w_down": normal_values(key_list[12], (FF, D), FF ** -0.5, 0.046875, ((0, 128),)),
    }


epsilon = 1e-06

def norm_rows(resid, norm_gain):
    resid_f32 = resid.astype(jnp.float32)
    mean_sq = lax.optimization_barrier(jnp.mean(resid_f32 * resid_f32, axis=1, keepdims=True))
    return (resid_f32 * lax.rsqrt(mean_sq + epsilon) * norm_gain.astype(jnp.float32)).astype(jnp.bfloat16)

def reference(hidden_in, q_nope, q_rope, new_kv, cache_kv, lengths, w_uk, w_uv, w_out, norm_gain, w_gate, w_up, w_down):
    seq_count = hidden_in.shape[0]
    nope_part = q_nope.reshape(seq_count, H, NOPE).astype(jnp.float32)
    key_up = w_uk.reshape(KV_RANK, H, NOPE).astype(jnp.float32)
    q_lat = jnp.einsum('bhd,chd->bhc', nope_part, key_up).astype(jnp.bfloat16)
    queries = jnp.concatenate([q_lat, q_rope.reshape(seq_count, H, ROPE)], axis=2)
    score_scale = float(NOPE + ROPE) ** (-0.5)
    positions = jnp.arange(CACHE, dtype=jnp.int32)

    def attend(sequence_item):
        one_query, one_cache, one_new, one_length = sequence_item
        scores = jnp.dot(one_query, one_cache.T, preferred_element_type=jnp.float32) * score_scale
        scores = jnp.where(positions[None, :] < one_length, scores, -jnp.inf)
        own_score = jnp.dot(one_query, one_new, preferred_element_type=jnp.float32) * score_scale
        row_top = jnp.maximum(lax.optimization_barrier(jnp.max(scores, axis=1)), own_score)
        weights = jnp.exp(scores - row_top[:, None])
        own_weight = jnp.exp(own_score - row_top)
        denom_sum = lax.optimization_barrier(jnp.sum(weights, axis=1)) + own_weight
        softmax_w = (weights / denom_sum[:, None]).astype(jnp.bfloat16)
        own_prob = (own_weight / denom_sum).astype(jnp.bfloat16)
        mixture = jnp.dot(softmax_w, one_cache, preferred_element_type=jnp.float32)
        mixture = mixture + own_prob.astype(jnp.float32)[:, None] * one_new.astype(jnp.float32)[None, :]
        return mixture[:, :KV_RANK].astype(jnp.bfloat16)
    latent = lax.map(attend, (queries, cache_kv, new_kv, lengths))
    value_up = w_uv.reshape(KV_RANK, H, VH).astype(jnp.float32)
    head_out = jnp.einsum('bhc,che->bhe', latent.astype(jnp.float32), value_up).astype(jnp.bfloat16)
    attn_out = jnp.dot(head_out.reshape(seq_count, H * VH), w_out, preferred_element_type=jnp.float32)
    resid = (hidden_in.astype(jnp.float32) + attn_out).astype(jnp.bfloat16)
    normed = norm_rows(resid, norm_gain)
    gate_val = jnp.dot(normed, w_gate, preferred_element_type=jnp.float32)
    up_val = jnp.dot(normed, w_up, preferred_element_type=jnp.float32)
    activated = (jax.nn.silu(gate_val) * up_val).astype(jnp.bfloat16)
    mlp_out = jnp.dot(activated, w_down, preferred_element_type=jnp.float32)
    return (resid.astype(jnp.float32) + mlp_out).astype(jnp.bfloat16)
```

```python
import functools

import jax
import jax.numpy as jnp
from jax import lax
from jax.experimental import pallas as pl
from jax.experimental.pallas import tpu as pltpu
from jax.sharding import PartitionSpec as P

D = 7168
FF_OWN = 144
H = 64
NOPE = 128
ROPE = 64
VH = 128
KV_RANK = 512
CACHE = 4096
SEQ = 4
BLOCK = 1024
EPS = 1e-06
SCALE = float(NOPE + ROPE) ** (-0.5)
MESH = pl.DeviceIdType.MESH
F32 = jnp.float32
BF16 = jnp.bfloat16
NT = (((1,), (1,)), ((), ()))
VMEM_LIMIT = 62 * 1024 * 1024


def coordinates():
    r, g = lax.axis_index("rep"), lax.axis_index("grp")
    return dict(
        r=r, g=g, core=r % 2, y=(r // 2) * 2 + g // 16, x=(g // 4) % 4, z=g % 4
    )


def device_at(at, **moved):
    x, y, z = (moved.get(k, at[k]) for k in "xyz")
    return ((y // 2) * 2 + at["core"], ((y % 2) * 4 + x) * 4 + z)


class Copies:
    def __init__(self, send_sems, recv_sems):
        self.send, self.recv, self.used, self.all = send_sems, recv_sems, 0, []

    def start(self, src, dst, device):
        k = self.used
        self.used += 1
        copy = pltpu.make_async_remote_copy(
            src_ref=src,
            dst_ref=dst,
            send_sem=self.send.at[k],
            recv_sem=self.recv.at[k],
            device_id=device,
            device_id_type=MESH,
        )
        copy.start()
        self.all.append(copy)
        return copy

    def finish(self):
        for copy in self.all:
            copy.wait_send()


def barrier_with(peers):
    sem = pltpu.get_barrier_semaphore()
    for peer in peers:
        pl.semaphore_signal(sem, inc=1, device_id=peer, device_id_type=MESH)
    pl.semaphore_wait(sem, len(peers))


class GatherRing:
    def __init__(self, copies, block, me, left, right, cut):
        self.copies, self.block, self.me = copies, block, me
        self.left, self.right, self.cut = left, right, cut

    def go(self, j, half, device):
        ref = self.block(j, self.cut[half])
        return self.copies.start(ref, ref, device)

    def start(self):
        m = self.me
        self.ra = self.go(m, 0, self.right)
        self.lb = self.go(m, 1, self.left)
        self.rb = self.go(m, 1, self.right)
        self.la = self.go(m, 0, self.left)

    def middle(self):
        m = self.me
        self.ra.wait_recv()
        self.rf = self.go((m + 3) % 4, 0, self.right)
        self.lb.wait_recv()
        self.lf = self.go((m + 1) % 4, 1, self.left)

    def end(self):
        for copy in (self.rb, self.la, self.rf, self.lf):
            copy.wait_recv()


class ScatterRing:
    def __init__(self, copies, src, landing, passing, me, left, right, cut):
        self.copies, self.src, self.landing, self.passing = copies, src, landing, passing
        self.me, self.left, self.right, self.cut = me, left, right, cut

    def part(self, j, half):
        start, size = self.cut[half]
        return self.src.at[j, :, pl.ds(start, size)]

    def land(self, k, half):
        return self.landing.at[k, :, pl.ds(0, self.cut[half][1])]

    def start(self):
        m, go = self.me, self.copies.start
        self.r0 = go(self.part((m + 2) % 4, 0), self.land(0, 0), self.right)
        self.l0 = go(self.part((m + 2) % 4, 1), self.land(1, 1), self.left)
        self.r1 = go(self.part((m + 1) % 4, 1), self.land(2, 1), self.right)
        self.l1 = go(self.part((m + 3) % 4, 0), self.land(3, 0), self.left)

    def value(self, ref):
        return ref[...].astype(F32)

    def middle(self):
        m, go = self.me, self.copies.start
        self.r0.wait_recv()
        held = self.passing.at[0, :, pl.ds(0, self.cut[0][1])]
        held[...] = (self.value(self.part((m + 1) % 4, 0)) + self.value(self.land(0, 0))).astype(BF16)
        self.r2 = go(held, self.land(4, 0), self.right)
        self.l0.wait_recv()
        held = self.passing.at[1, :, pl.ds(0, self.cut[1][1])]
        held[...] = (self.value(self.part((m + 3) % 4, 1)) + self.value(self.land(1, 1))).astype(BF16)
        self.l2 = go(held, self.land(5, 1), self.left)

    def end(self):
        m = self.me
        self.l1.wait_recv()
        self.r2.wait_recv()
        first = self.value(self.part(m, 0)) + self.value(self.land(4, 0)) + self.value(self.land(3, 0))
        self.r1.wait_recv()
        self.l2.wait_recv()
        second = self.value(self.part(m, 1)) + self.value(self.land(2, 1)) + self.value(self.land(5, 1))
        return first, second


def query_kernel(q_ref, wuk_ref, wuv_ref, out_ref, wuv_out, gathered, rows, made, own_sem, send_sems, recv_sems):
    at = coordinates()
    r, g = at["r"], at["g"]
    peers = [((r + k) % 4, g) for k in (1, 2, 3)]
    barrier_with(peers)
    copies = Copies(send_sems, recv_sems)
    mine = wuv_ref.at[:, pl.ds(pl.multiple_of(g * 256, 256), 256)]
    incoming = [copies.start(q_ref, gathered.at[r], peer) for peer in peers]
    own = pltpu.make_async_copy(mine, wuv_out.at[r], own_sem)
    own.start()
    weights = [copies.start(mine, wuv_out.at[r], peer) for peer in peers]
    gathered[r] = q_ref[...]
    for copy in incoming:
        copy.wait_recv()
    for s in range(4):
        rows[pl.ds(4 * s, 4), :] = gathered[s].astype(F32)

    def heads(i, carry):
        for k in range(8):
            h = i * 8 + k
            cols = pl.ds(pl.multiple_of(h * NOPE, NOPE), NOPE)
            lat = lax.dot_general(
                rows[:, cols].astype(BF16), wuk_ref[:, cols], NT, preferred_element_type=F32
            )
            for s in range(4):
                made[s, h] = lat[4 * s : 4 * s + 4].astype(BF16)
        return carry

    lax.fori_loop(0, H // 8, heads, 0)
    back = [copies.start(made.at[peer[0]], out_ref.at[r], peer) for peer in peers]
    out_ref[r] = made[r]
    for copy in back + weights:
        copy.wait_recv()
    own.wait()
    copies.finish()


def spread_queries(q_nope, w_uk, w_uv):
    return pl.pallas_call(
        query_kernel,
        out_shape=(
            jax.ShapeDtypeStruct((4, H, SEQ, NOPE), BF16),
            jax.ShapeDtypeStruct((4, 128, 256), BF16),
        ),
        in_specs=[
            pl.BlockSpec(memory_space=pltpu.VMEM),
            pl.BlockSpec(memory_space=pltpu.VMEM),
            pl.BlockSpec(memory_space=pl.ANY),
        ],
        out_specs=(
            pl.BlockSpec(memory_space=pltpu.VMEM),
            pl.BlockSpec(memory_space=pl.ANY),
        ),
        scratch_shapes=[
            pltpu.VMEM((4, SEQ, H * NOPE), BF16),
            pltpu.VMEM((16, H * NOPE), F32),
            pltpu.VMEM((4, H, SEQ, NOPE), BF16),
            pltpu.SemaphoreType.DMA,
            pltpu.SemaphoreType.DMA((9,)),
            pltpu.SemaphoreType.DMA((9,)),
        ],
        compiler_params=pltpu.CompilerParams(
            collective_id=0, has_side_effects=True, vmem_limit_bytes=VMEM_LIMIT
        ),
        name="spread_queries",
    )(q_nope, w_uk, w_uv)


def attention_kernel(len_ref, q_ref, new_ref, kt_ref, out_ref, top, total, mix):
    b, k = pl.program_id(0), pl.program_id(1)
    length = len_ref[b]

    @pl.when(k == 0)
    def _():
        new = new_ref[0].astype(F32)
        own = jnp.sum(q_ref[0].astype(F32) * new, axis=1, keepdims=True) * SCALE
        top[...] = own
        total[...] = jnp.ones_like(own)
        mix[...] = jnp.broadcast_to(new[:, :KV_RANK], (H, KV_RANK))

    @pl.when(k * BLOCK < length)
    def _():
        s = jnp.dot(q_ref[0], kt_ref[0], preferred_element_type=F32) * SCALE
        pos = lax.broadcasted_iota(jnp.int32, s.shape, 1) + k * BLOCK
        s = jnp.where(pos < length, s, -jnp.inf)
        high = jnp.maximum(top[...], jnp.max(s, axis=1, keepdims=True))
        p = jnp.exp(s - high)
        fade = jnp.exp(top[...] - high)
        total[...] = total[...] * fade + jnp.sum(p, axis=1, keepdims=True)
        top[...] = high
        mix[...] = mix[...] * fade + lax.dot_general(
            p.astype(BF16), kt_ref[0, :KV_RANK, :], NT, preferred_element_type=F32
        )

    @pl.when(k == CACHE // BLOCK - 1)
    def _():
        out_ref[0] = (mix[...] / total[...]).astype(BF16)


def attend(lengths, queries, new_kv, cache_t):
    width = KV_RANK + ROPE
    return pl.pallas_call(
        attention_kernel,
        out_shape=jax.ShapeDtypeStruct((SEQ, H, KV_RANK), BF16),
        grid_spec=pltpu.PrefetchScalarGridSpec(
            num_scalar_prefetch=1,
            grid=(SEQ, CACHE // BLOCK),
            in_specs=[
                pl.BlockSpec((1, H, width), lambda b, k, n: (b, 0, 0)),
                pl.BlockSpec((1, 1, width), lambda b, k, n: (b, 0, 0)),
                pl.BlockSpec(
                    (1, width, BLOCK),
                    lambda b, k, n: (b, 0, jnp.minimum(k, (n[b] - 1) // BLOCK)),
                ),
            ],
            out_specs=pl.BlockSpec((1, H, KV_RANK), lambda b, k, n: (b, 0, 0)),
            scratch_shapes=[
                pltpu.VMEM((H, 1), F32),
                pltpu.VMEM((H, 1), F32),
                pltpu.VMEM((H, KV_RANK), F32),
            ],
        ),
        compiler_params=pltpu.CompilerParams(vmem_limit_bytes=VMEM_LIMIT),
        name="attend",
    )(lengths, queries, new_kv, cache_t)


HALF = D // 2
HALF_CUT = ((0, HALF // 2), (HALF // 2, HALF // 2))


def iota(shape, dim):
    return lax.broadcasted_iota(jnp.int32, shape, dim)


def project_kernel(
    lat_ref, wuv_ref, wout_ref, hidden_ref, gain_ref, wg_ref, wu_ref, wd_ref,
    resid_ref, normed_ref, others_ref,
    got, part_a, part_b, next_a, next_b, last_a, last_b,
    land_a1, land_b1, land_a2, land_b2, pass_a1, pass_b1, pass_a2, pass_b2, land_a3, land_b3,
    send_sems, recv_sems,
):
    at = coordinates()
    r, g, x, z = at["r"], at["g"], at["x"], at["z"]
    y_lo = g // 16
    peers = [(r, (g + k) % 32) for k in range(1, 32)]
    twin = (r + 1 - 2 * at["core"], g)
    barrier_with(peers + [twin])
    copies = Copies(send_sems, recv_sems)
    incoming = [copies.start(lat_ref.at[peer[1]], got.at[g], peer) for peer in peers]
    traded = [
        copies.start(ref, others_ref.at[i], twin) for i, ref in enumerate((wg_ref, wu_ref, wd_ref))
    ]
    got[g] = lat_ref[g]
    for copy in incoming:
        copy.wait_recv()

    heads = jnp.dot(got[...].reshape(256, KV_RANK), wuv_ref[...], preferred_element_type=F32)
    row, col = iota((256, 256), 0), iota((256, 256), 1)
    heads = jnp.where((row & 1) == (col >> 7), heads, 0.0).astype(BF16)
    row, col = iota((128, 256), 0), iota((128, 256), 1)
    b, y_of, low, high = row & 3, (row >> 2) & 1, (row >> 3) & 3, row >> 5

    def project(x_of, z_of, part, first_col):
        source = (((y_of * 4 + x_of) * 4) + z_of) * 4 + b
        pick = jnp.where((col >> 1) == source, 1.0, 0.0).astype(BF16)
        rows = jnp.dot(pick, heads, preferred_element_type=F32).astype(BF16)
        step = HALF // 4
        for n in range(4):
            out = jnp.dot(
                rows, wout_ref[:, pl.ds(first_col + n * step, step)], preferred_element_type=F32
            )
            part[:, :, pl.ds(n * step, step)] = out.astype(BF16).reshape(4, 32, step)

    def ring(axis, src, landing, passing):
        m = at[axis]
        left = device_at(at, **{axis: (m + 3) % 4})
        right = device_at(at, **{axis: (m + 1) % 4})
        return ScatterRing(copies, src, landing, passing, m, left, right, HALF_CUT)

    project(high, low, part_a, 0)
    a1 = ring("x", part_a, land_a1, pass_a1)
    a1.start()
    project(low, high, part_b, HALF)
    b1 = ring("z", part_b, land_b1, pass_b1)
    b1.start()
    a1.middle()
    b1.middle()

    def hand_on(values, ref, count):
        rows = values[0].shape[0] // count
        for (start, size), value in zip(HALF_CUT, values):
            for j in range(count):
                ref[j, :, pl.ds(start, size)] = value[j * rows : (j + 1) * rows].astype(BF16)

    hand_on(a1.end(), next_a, 4)
    a2 = ring("z", next_a, land_a2, pass_a2)
    a2.start()
    hand_on(b1.end(), next_b, 4)
    b2 = ring("x", next_b, land_b2, pass_b2)
    b2.start()
    a2.middle()
    b2.middle()
    across = (r, (g + 16) % 32)
    hand_on(a2.end(), last_a, 2)
    a3 = copies.start(last_a.at[1 - y_lo], land_a3, across)
    hand_on(b2.end(), last_b, 2)
    b3 = copies.start(last_b.at[1 - y_lo], land_b3, across)
    squares = jnp.zeros((SEQ, 1), F32)
    kept = []
    for i, (copy, last, landing) in enumerate(((a3, last_a, land_a3), (b3, last_b, land_b3))):
        copy.wait_recv()
        cols = pl.ds(i * HALF, HALF)
        total = last[y_lo].astype(F32) + landing[...].astype(F32) + hidden_ref[:, cols].astype(F32)
        resid = total.astype(BF16)
        resid_ref[:, cols] = resid
        resid = resid.astype(F32)
        kept.append(resid)
        squares += jnp.sum(resid * resid, axis=1, keepdims=True)
    factor = lax.rsqrt(squares / D + EPS)
    for i in range(2):
        cols = pl.ds(i * HALF, HALF)
        normed_ref[:, cols] = (kept[i] * factor * gain_ref[:, cols].astype(F32)).astype(BF16)
    for copy in traded:
        copy.wait_recv()
    copies.finish()


def project_heads(lat, wuv, w_out, hidden_in, gain, wg_t, wu_t, wd):
    vmem = pl.BlockSpec(memory_space=pltpu.VMEM)
    hbm = pl.BlockSpec(memory_space=pl.ANY)
    count = 31 + 3 + 2 * 13
    half = HALF // 2
    return pl.pallas_call(
        project_kernel,
        out_shape=(
            jax.ShapeDtypeStruct((SEQ, D), BF16),
            jax.ShapeDtypeStruct((SEQ, D), BF16),
            jax.ShapeDtypeStruct((3, FF_OWN, D), BF16),
        ),
        in_specs=[vmem] * 5 + [hbm] * 3,
        out_specs=(vmem, vmem, hbm),
        scratch_shapes=[pltpu.VMEM((32, 8, KV_RANK), BF16)]
        + [pltpu.VMEM((4, 32, HALF), BF16)] * 2
        + [pltpu.VMEM((4, 8, HALF), BF16)] * 2
        + [pltpu.VMEM((2, 4, HALF), BF16)] * 2
        + [pltpu.VMEM((6, 32, half), BF16)] * 2
        + [pltpu.VMEM((6, 8, half), BF16)] * 2
        + [pltpu.VMEM((2, 32, half), BF16)] * 2
        + [pltpu.VMEM((2, 8, half), BF16)] * 2
        + [pltpu.VMEM((4, HALF), BF16)] * 2
        + [pltpu.SemaphoreType.DMA((count,)), pltpu.SemaphoreType.DMA((count,))],
        compiler_params=pltpu.CompilerParams(
            collective_id=1, has_side_effects=True, vmem_limit_bytes=VMEM_LIMIT
        ),
        name="project_heads",
    )(lat, wuv, w_out, hidden_in, gain, wg_t, wu_t, wd)


WIDTHS = (2432, 2432, 2304)
STARTS = (0, 2432, 4864)
CUTS = tuple(
    ((0, (w // 256) * 128 + (w % 256)), ((w // 256) * 128 + (w % 256), (w // 256) * 128)) for w in WIDTHS
)
AXES = (("x", "y", "z"), ("y", "z", "x"), ("z", "x", "y"))


def mlp_kernel(
    normed_ref, resid_ref, wg_ref, wu_ref, wd_ref, others_ref, out_ref,
    gates, downs, sums, turned, *rest,
):
    rest = list(rest)

    def take(n):
        taken, rest[:n] = rest[:n], []
        return taken

    slots, blocks, all_rows = take(3), take(3), take(3)
    parts, nexts, lasts = take(3), take(3), take(3)
    landings = [take(3) for _ in range(3)]
    passings = [take(3) for _ in range(3)]
    local_sems, send_sems, recv_sems = take(3)

    at = coordinates()
    peers = []
    for axis in "xyz":
        for step in (1, 3):
            peers.append(device_at(at, **{axis: (at[axis] + step) % 4}))
    loads = []
    for i, (src, dst) in enumerate(
        (
            (wg_ref, gates.at[0]),
            (others_ref.at[0], gates.at[1]),
            (wu_ref, gates.at[2]),
            (others_ref.at[1], gates.at[3]),
            (wd_ref, downs.at[0]),
            (others_ref.at[2], downs.at[1]),
        )
    ):
        loads.append(pltpu.make_async_copy(src, dst, local_sems.at[i]))
        loads[-1].start()
    barrier_with(peers)
    copies = Copies(send_sems, recv_sems)

    def sides(axis):
        m = at[axis]
        return m, device_at(at, **{axis: (m + 3) % 4}), device_at(at, **{axis: (m + 1) % 4})

    def run(rings):
        for ring in rings:
            ring.start()
        for ring in rings:
            ring.middle()

    def gather(p, axis, block):
        return GatherRing(copies, block, *sides(axis), CUTS[p])

    rings = []
    for p in range(3):
        a, b, c = AXES[p]
        slots[p][at[c]] = normed_ref[:, pl.ds(STARTS[p], WIDTHS[p])]
        ref = slots[p]
        rings.append(gather(p, c, lambda j, cut, ref=ref: ref.at[j, :, pl.ds(*cut)]))
    run(rings)
    later = []
    for p in range(3):
        a, b, c = AXES[p]
        rings[p].end()
        for s in range(4):
            blocks[p][pl.ds(4 * s, 4), :] = slots[p][s].astype(F32)
        all_rows[p][at[a], at[b]] = blocks[p][...].astype(BF16)
        ref = all_rows[p].at[at[a]]
        later.append(gather(p, b, lambda j, cut, ref=ref: ref.at[j, :, pl.ds(*cut)]))
        later[p].start()
    rings = later
    for ring in rings:
        ring.middle()
    later = []
    for p in range(3):
        rings[p].end()
        ref = all_rows[p]
        later.append(gather(p, AXES[p][0], lambda j, cut, ref=ref: ref.at[j, :, :, pl.ds(*cut)]))
        later[p].start()
    for ring in later:
        ring.middle()

    row, col = iota((256, 256), 0), iota((256, 256), 1)

    def place(p, i):
        b = i & 3
        of = {"z": (i >> 2) & 3, "y": (i >> 4) & 3, "x": (i >> 6) & 3}
        s, t, u = (of[axis] for axis in AXES[p])
        return ((s * 4 + t) * 4 + u) * 4 + b

    for load in loads[:4]:
        load.wait()
    for p in range(3):
        later[p].end()
        rows = all_rows[p][...].reshape(256, WIDTHS[p])
        if p > 0:
            order = jnp.where(col == place(p, row), 1.0, 0.0).astype(BF16)
            rows = jnp.dot(order, rows, preferred_element_type=F32).astype(BF16)
        weights = gates[:, :, pl.ds(STARTS[p], WIDTHS[p])].reshape(4 * FF_OWN, WIDTHS[p])
        product = lax.dot_general(weights, rows, NT, preferred_element_type=F32)
        if p > 0:
            product += sums[...]
        sums[...] = product
    gate, up = sums[pl.ds(0, 2 * FF_OWN), :], sums[pl.ds(2 * FF_OWN, 2 * FF_OWN), :]
    turned[...] = (gate / (1.0 + jnp.exp(-gate)) * up).astype(BF16)

    for load in loads[4:]:
        load.wait()

    def scatter(p, axis, phase, src):
        return ScatterRing(copies, src, landings[phase][p], passings[phase][p], *sides(axis), CUTS[p])

    rings = []
    for p in range(3):
        order = jnp.where(row == place(p, col), 1.0, 0.0).astype(BF16)
        act = lax.dot_general(order, turned[...], NT, preferred_element_type=F32).astype(BF16)
        for start, size in CUTS[p]:
            weights = downs[:, :, pl.ds(STARTS[p] + start, size)].reshape(2 * FF_OWN, size)
            out = jnp.dot(act, weights, preferred_element_type=F32)
            parts[p][:, :, pl.ds(start, size)] = out.astype(BF16).reshape(4, 64, size)
        rings.append(scatter(p, AXES[p][0], 0, parts[p]))
        rings[p].start()
    for ring in rings:
        ring.middle()

    def hand_on(p, values, ref):
        rows = values[0].shape[0] // 4
        for (start, size), value in zip(CUTS[p], values):
            for j in range(4):
                ref[j, :, pl.ds(start, size)] = value[j * rows : (j + 1) * rows].astype(BF16)

    for phase, targets in ((1, nexts), (2, lasts)):
        later = []
        for p in range(3):
            hand_on(p, rings[p].end(), targets[p])
            later.append(scatter(p, AXES[p][phase], phase, targets[p]))
            later[p].start()
        rings = later
        for ring in rings:
            ring.middle()
    for p in range(3):
        for (start, size), value in zip(CUTS[p], rings[p].end()):
            cols = pl.ds(STARTS[p] + start, size)
            out_ref[:, cols] = (value + resid_ref[:, cols].astype(F32)).astype(BF16)
    copies.finish()


def mlp(normed, resid, wg_t, wu_t, wd, others):
    vmem = pl.BlockSpec(memory_space=pltpu.VMEM)
    hbm = pl.BlockSpec(memory_space=pl.ANY)
    halves = [cut[0][1] for cut in CUTS]
    scratch = [
        pltpu.VMEM((4, FF_OWN, D), BF16),
        pltpu.VMEM((2, FF_OWN, D), BF16),
        pltpu.VMEM((4 * FF_OWN, 256), F32),
        pltpu.VMEM((2 * FF_OWN, 256), BF16),
    ]
    scratch += [pltpu.VMEM((4, 4, w), BF16) for w in WIDTHS]
    scratch += [pltpu.VMEM((16, w), F32) for w in WIDTHS]
    scratch += [pltpu.VMEM((4, 4, 16, w), BF16) for w in WIDTHS]
    for rows in (64, 16, 4):
        scratch += [pltpu.VMEM((4, rows, w), BF16) for w in WIDTHS]
    for rows in (64, 16, 4):
        scratch += [pltpu.VMEM((6, rows, h), BF16) for h in halves]
    for rows in (64, 16, 4):
        scratch += [pltpu.VMEM((2, rows, h), BF16) for h in halves]
    count = 2 * 3 * 3 * 6
    scratch += [pltpu.SemaphoreType.DMA((n,)) for n in (6, count, count)]
    return pl.pallas_call(
        mlp_kernel,
        out_shape=jax.ShapeDtypeStruct((SEQ, D), BF16),
        in_specs=[vmem] * 2 + [hbm] * 4,
        out_specs=vmem,
        scratch_shapes=scratch,
        compiler_params=pltpu.CompilerParams(
            collective_id=2, has_side_effects=True, vmem_limit_bytes=VMEM_LIMIT
        ),
        name="mlp",
    )(normed, resid, wg_t, wu_t, wd, others)


def on_device(
    hidden_in, q_nope, q_rope, new_kv, cache_kv, lengths,
    w_uk, w_uv, w_out, norm_gain, w_gate, w_up, w_down,
):
    q_lat, value_up = spread_queries(q_nope, w_uk, w_uv)
    q_lat = jnp.transpose(q_lat, (2, 1, 0, 3)).reshape(SEQ, H, KV_RANK)
    queries = jnp.concatenate([q_lat, q_rope.reshape(SEQ, H, ROPE)], axis=2)
    latent = attend(lengths, queries, new_kv[:, None, :], jnp.swapaxes(cache_kv, 1, 2))
    latent = jnp.transpose(latent.reshape(SEQ, 32, 2, KV_RANK), (1, 0, 2, 3)).reshape(32, 8, KV_RANK)
    wg_t, wu_t = w_gate.T, w_up.T
    resid, normed, others = project_heads(
        latent, value_up.reshape(KV_RANK, 256), w_out, hidden_in, norm_gain[None, :], wg_t, wu_t, w_down
    )
    return mlp(normed, resid, wg_t, wu_t, w_down, others)


def solution(mesh):
    return jax.shard_map(
        on_device,
        mesh=mesh,
        in_specs=(
            P(("rep", "grp"), None),
            P(("rep", "grp"), None),
            P(("rep", "grp"), None),
            P(("rep", "grp"), None),
            P(("rep", "grp"), None, None),
            P(("rep", "grp")),
            P("rep", None),
            P("rep", None),
            P("grp", None),
            P(),
            P(None, ("rep", "grp")),
            P(None, ("rep", "grp")),
            P(("rep", "grp"), None),
        ),
        out_specs=P(("rep", "grp"), None),
        check_vma=False,
    )
```

```python
import functools

import jax
import jax.numpy as jnp
from jax import lax
from jax.experimental import pallas as pl
from jax.experimental.pallas import tpu as pltpu
from jax.sharding import PartitionSpec as P

D = 7168
FF_OWN = 144
H = 64
NOPE = 128
ROPE = 64
VH = 128
KV_RANK = 512
CACHE = 4096
SEQ = 4
BLOCK = 1024
EPS = 1e-06
SCALE = float(NOPE + ROPE) ** (-0.5)
MESH = pl.DeviceIdType.MESH
F32 = jnp.float32
BF16 = jnp.bfloat16
NT = (((1,), (1,)), ((), ()))
VMEM_LIMIT = 62 * 1024 * 1024


def coordinates():
    r, g = lax.axis_index("rep"), lax.axis_index("grp")
    return dict(
        r=r, g=g, core=r % 2, y=(r // 2) * 2 + g // 16, x=(g // 4) % 4, z=g % 4
    )


def device_at(at, **moved):
    x, y, z = (moved.get(k, at[k]) for k in "xyz")
    return ((y // 2) * 2 + at["core"], ((y % 2) * 4 + x) * 4 + z)


class Copies:
    def __init__(self, send_sems, recv_sems):
        self.send, self.recv, self.used, self.all = send_sems, recv_sems, 0, []

    def start(self, src, dst, device):
        k = self.used
        self.used += 1
        copy = pltpu.make_async_remote_copy(
            src_ref=src,
            dst_ref=dst,
            send_sem=self.send.at[k],
            recv_sem=self.recv.at[k],
            device_id=device,
            device_id_type=MESH,
        )
        copy.start()
        self.all.append(copy)
        return copy

    def finish(self):
        for copy in self.all:
            copy.wait_send()


def barrier_with(peers):
    sem = pltpu.get_barrier_semaphore()
    for peer in peers:
        pl.semaphore_signal(sem, inc=1, device_id=peer, device_id_type=MESH)
    pl.semaphore_wait(sem, len(peers))


class GatherRing:
    def __init__(self, copies, block, side, cut):
        self.copies, self.block, self.cut = copies, block, cut
        self.me, self.left, self.right = side

    def go(self, j, half, device):
        ref = self.block(j, self.cut[half])
        return self.copies.start(ref, ref, device)

    def start(self):
        m = self.me
        self.ra = self.go(m, 0, self.right)
        self.lb = self.go(m, 1, self.left)
        self.rb = self.go(m, 1, self.right)
        self.la = self.go(m, 0, self.left)

    def middle(self):
        m = self.me
        self.ra.wait_recv()
        self.rf = self.go((m + 3) % 4, 0, self.right)
        self.lb.wait_recv()
        self.lf = self.go((m + 1) % 4, 1, self.left)

    def near(self):
        self.rb.wait_recv()
        self.la.wait_recv()

    def far(self):
        self.rf.wait_recv()
        self.lf.wait_recv()


class ScatterRing:
    def __init__(self, copies, chunk, landing, passing, side, cut):
        self.copies, self.chunk, self.landing, self.passing, self.cut = copies, chunk, landing, passing, cut
        self.me, self.left, self.right = side

    def part(self, step, half):
        return self.chunk((self.me + step) % 4, self.cut[half])

    def land(self, k, half):
        return self.landing.at[k, :, pl.ds(0, self.cut[half][1])]

    def send_far(self):
        go = self.copies.start
        self.r0 = go(self.part(2, 0), self.land(0, 0), self.right)
        self.l0 = go(self.part(2, 1), self.land(1, 1), self.left)

    def send_right(self):
        self.r1 = self.copies.start(self.part(1, 1), self.land(2, 1), self.right)

    def send_left(self):
        self.l1 = self.copies.start(self.part(3, 0), self.land(3, 0), self.left)

    def start(self):
        self.send_far()
        self.send_right()
        self.send_left()

    def value(self, ref):
        return ref[...].astype(F32)

    def pass_on(self, copy, step, half, device):
        copy.wait_recv()
        held = self.passing.at[half, :, pl.ds(0, self.cut[half][1])]
        held[...] = (self.value(self.part(step, half)) + self.value(self.land(half, half))).astype(BF16)
        return self.copies.start(held, self.land(4 + half, half), device)

    def middle(self):
        self.r2 = self.pass_on(self.r0, 1, 0, self.right)
        self.l2 = self.pass_on(self.l0, 3, 1, self.left)

    def end(self):
        self.l1.wait_recv()
        self.r2.wait_recv()
        first = self.value(self.part(0, 0)) + self.value(self.land(4, 0)) + self.value(self.land(3, 0))
        self.r1.wait_recv()
        self.l2.wait_recv()
        second = self.value(self.part(0, 1)) + self.value(self.land(2, 1)) + self.value(self.land(5, 1))
        return first, second


GROUP = 16


def query_kernel(
    q_ref, rope_ref, wuk_hbm, wuv_ref, out_ref, wuv_out,
    gathered, rows, wuk, tall, made, own_sem, load_sems, send_sems, recv_sems,
):
    at = coordinates()
    r, g = at["r"], at["g"]
    wide = GROUP * NOPE
    spans = [pl.ds(i * wide, wide) for i in range(H // GROUP)]
    loads = [
        pltpu.make_async_copy(wuk_hbm.at[:, span], wuk.at[:, span], load_sems.at[i])
        for i, span in enumerate(spans)
    ]
    for load in loads:
        load.start()
    mine = wuv_ref.at[:, pl.ds(pl.multiple_of(g * 256, 256), 256)]
    own = pltpu.make_async_copy(mine, wuv_out.at[r], own_sem)
    own.start()
    peers = [((r + k) % 4, g) for k in (1, 2, 3)]
    barrier_with(peers)
    copies = Copies(send_sems, recv_sems)
    incoming = [
        [copies.start(q_ref.at[:, span], gathered.at[r, :, span], peer) for peer in peers] for span in spans
    ]
    gathered[r] = q_ref[...]
    out_ref[:, :, pl.ds(KV_RANK, ROPE)] = rope_ref[...]
    slice_of_rank = pl.ds(pl.multiple_of(r * NOPE, NOPE), NOPE)
    back = []
    for i, span in enumerate(spans):
        for copy in incoming[i]:
            copy.wait_recv()
        loads[i].wait()
        for s in range(4):
            rows[pl.ds(4 * s, 4), :] = gathered[s, :, span].astype(F32)
        for k in range(GROUP):
            lat = lax.dot_general(
                rows[:, pl.ds(k * NOPE, NOPE)].astype(BF16),
                wuk[:, pl.ds((i * GROUP + k) * NOPE, NOPE)],
                NT,
                preferred_element_type=F32,
            )
            tall[:, k, :] = lat
        heads = pl.ds(i * GROUP, GROUP)
        made[:, :, heads, :] = tall[...].astype(BF16).reshape(4, SEQ, GROUP, NOPE)
        for peer in peers:
            back.append(
                copies.start(made.at[peer[0], :, heads, :], out_ref.at[:, heads, slice_of_rank], peer)
            )
    weights = [copies.start(mine, wuv_out.at[r], peer) for peer in peers]
    out_ref[:, :, slice_of_rank] = made[r]
    for copy in back + weights:
        copy.wait_recv()
    own.wait()
    copies.finish()


def spread_queries(q_nope, q_rope, w_uk, w_uv):
    vmem = pl.BlockSpec(memory_space=pltpu.VMEM)
    hbm = pl.BlockSpec(memory_space=pl.ANY)
    count = 3 + 6 * (H // GROUP)
    return pl.pallas_call(
        query_kernel,
        out_shape=(
            jax.ShapeDtypeStruct((SEQ, H, KV_RANK + ROPE), BF16),
            jax.ShapeDtypeStruct((4, 128, 256), BF16),
        ),
        in_specs=[vmem, vmem, hbm, hbm],
        out_specs=(vmem, hbm),
        scratch_shapes=[
            pltpu.VMEM((4, SEQ, H * NOPE), BF16),
            pltpu.VMEM((16, GROUP * NOPE), F32),
            pltpu.VMEM((128, H * NOPE), BF16),
            pltpu.VMEM((16, GROUP, NOPE), F32),
            pltpu.VMEM((4, SEQ, H, NOPE), BF16),
            pltpu.SemaphoreType.DMA,
            pltpu.SemaphoreType.DMA((H // GROUP,)),
            pltpu.SemaphoreType.DMA((count,)),
            pltpu.SemaphoreType.DMA((count,)),
        ],
        compiler_params=pltpu.CompilerParams(
            collective_id=0, has_side_effects=True, vmem_limit_bytes=VMEM_LIMIT
        ),
        name="spread_queries",
    )(q_nope, q_rope, w_uk, w_uv)


def attention_kernel(len_ref, q_ref, new_ref, kt_ref, out_ref, scores, lanes, mixed):
    b = pl.program_id(0)
    length = len_ref[b]
    q = q_ref[0]
    pick = lax.broadcasted_iota(jnp.int32, new_ref.shape, 0) == b
    new = jnp.sum(jnp.where(pick, new_ref[...].astype(F32), 0.0), axis=0, keepdims=True)
    own = jnp.sum(q.astype(F32) * new, axis=1, keepdims=True) * SCALE
    lane = lax.broadcasted_iota(jnp.int32, (H, BLOCK), 1)
    top = jnp.full((H, 128), -jnp.inf, F32)
    for c in range(CACHE // BLOCK):
        cols = pl.ds(c * BLOCK, BLOCK)
        s = jnp.dot(q, kt_ref[0, :, cols], preferred_element_type=F32) * SCALE
        s = jnp.where(lane < length - c * BLOCK, s, -jnp.inf)
        scores[:, cols] = s
        for i in range(BLOCK // 128):
            top = jnp.maximum(top, s[:, i * 128 : (i + 1) * 128])
    top = jnp.maximum(jnp.max(top, axis=1, keepdims=True), own)
    own = jnp.exp(own - top)
    total = jnp.zeros((H, 128), F32)
    mix = own * new[:, :KV_RANK]
    for c in range(CACHE // BLOCK):
        cols = pl.ds(c * BLOCK, BLOCK)
        p = jnp.exp(scores[:, cols] - top)
        for i in range(BLOCK // 128):
            total += p[:, i * 128 : (i + 1) * 128]
        mix += lax.dot_general(
            p.astype(BF16), kt_ref[0, :KV_RANK, cols], NT, preferred_element_type=F32
        )
    mix = mix / (jnp.sum(total, axis=1, keepdims=True) + own)
    for t in range(KV_RANK // 128):
        lanes[t] = mix[:, t * 128 : (t + 1) * 128]
        for h in range(2):
            mixed[t, :, 2 * b + h, :] = lanes[t, pl.ds(h, H // 2, stride=2), :]

    @pl.when(b == SEQ - 1)
    def _():
        for t in range(KV_RANK // 128):
            out_ref[:, :, pl.ds(t * 128, 128)] = mixed[t].astype(BF16)


def attend(lengths, queries, new_kv, cache_t):
    width = KV_RANK + ROPE
    return pl.pallas_call(
        attention_kernel,
        out_shape=jax.ShapeDtypeStruct((H // 2, 2 * SEQ, KV_RANK), BF16),
        grid_spec=pltpu.PrefetchScalarGridSpec(
            num_scalar_prefetch=1,
            grid=(SEQ,),
            in_specs=[
                pl.BlockSpec((1, H, width), lambda b, n: (b, 0, 0)),
                pl.BlockSpec((SEQ, width), lambda b, n: (0, 0)),
                pl.BlockSpec((1, width, CACHE), lambda b, n: (b, 0, 0)),
            ],
            out_specs=pl.BlockSpec((H // 2, 2 * SEQ, KV_RANK), lambda b, n: (0, 0, 0)),
            scratch_shapes=[
                pltpu.VMEM((H, CACHE), F32),
                pltpu.VMEM((KV_RANK // 128, H, 128), F32),
                pltpu.VMEM((KV_RANK // 128, H // 2, 2 * SEQ, 128), F32),
            ],
        ),
        compiler_params=pltpu.CompilerParams(vmem_limit_bytes=VMEM_LIMIT),
        name="attend",
    )(lengths, queries, new_kv, cache_t)


HALF = D // 2
HALF_CUT = ((0, HALF // 2), (HALF // 2, HALF // 2))
WIDTHS = (2432, 2432, 2304)
STARTS = (0, 2432, 4864)
CUTS = tuple(
    ((0, (w // 256) * 128 + (w % 256)), ((w // 256) * 128 + (w % 256), (w // 256) * 128)) for w in WIDTHS
)
AXES = (("x", "y", "z"), ("y", "z", "x"), ("z", "x", "y"))
STEPS = (2, 1, 3, 0)


def iota(shape, dim):
    return lax.broadcasted_iota(jnp.int32, shape, dim)


class Taker:
    def __init__(self, refs):
        self.refs = list(refs)

    def __call__(self, n):
        taken, self.refs = self.refs[:n], self.refs[n:]
        return taken


def layer_kernel(
    lat_ref, wuv_ref, wout_hbm, hidden_ref, gain_ref, wg_ref, wu_ref, wd_ref, out_ref,
    got, wout, gates, downs, sums, turned, resid_ref, *rest,
):
    take = Taker(rest)
    part2, next2, land2, last2, land1, pass1, landy = (take(2) for _ in range(7))
    slots, blocks, all_rows = take(3), take(3), take(3)
    parts, nexts, lasts = take(3), take(3), take(3)
    landings, passings, landings2, passings2, landings3 = (take(3) for _ in range(5))
    local_sems, send_sems, recv_sems = take(3)

    at = coordinates()
    r, g = at["r"], at["g"]
    y_lo = g // 16
    loads = []
    for i, (src, dst) in enumerate(
        ((wout_hbm, wout), (wg_ref, gates.at[0]), (wu_ref, gates.at[2]), (wd_ref, downs.at[0]))
    ):
        loads.append(pltpu.make_async_copy(src, dst, local_sems.at[i]))
        loads[-1].start()

    def peer_along(axis, step):
        return device_at(at, **{axis: (at[axis] + step) % 4})

    def side(axis):
        return at[axis], peer_along(axis, 3), peer_along(axis, 1)

    peers = [(r, (g + k) % 32) for k in range(1, 32)]
    twin = (r + 1 - 2 * at["core"], g)
    other = (r + 2) % 4
    barrier_with(peers + [twin, (other, g), (other, (g + 16) % 32)])
    copies = Copies(send_sems, recv_sems)
    incoming = [copies.start(lat_ref.at[peer[1]], got.at[g], peer) for peer in peers]
    traded = [
        copies.start(src, dst, twin)
        for src, dst in ((wg_ref, gates.at[1]), (wu_ref, gates.at[3]), (wd_ref, downs.at[1]))
    ]
    got[g] = lat_ref[g]
    for copy in incoming:
        copy.wait_recv()

    heads = jnp.dot(got[...].reshape(256, KV_RANK), wuv_ref[...], preferred_element_type=F32)
    row, col = iota((256, 256), 0), iota((256, 256), 1)
    heads = jnp.where((row & 1) == (col >> 7), heads, 0.0).astype(BF16)
    row, col = iota((128, 256), 0), iota((128, 256), 1)
    b, y_of, low, high = row & 3, (row >> 2) & 1, (row >> 3) & 3, row >> 5
    loads[0].wait()

    def project(x_of, z_of, part, first_col):
        source = (((y_of * 4 + x_of) * 4) + z_of) * 4 + b
        pick = jnp.where((col >> 1) == source, 1.0, 0.0).astype(BF16)
        rows = jnp.dot(pick, heads, preferred_element_type=F32).astype(BF16)
        step = HALF // 4
        for n in range(4):
            out = jnp.dot(
                rows, wout[:, pl.ds(first_col + n * step, step)], preferred_element_type=F32
            )
            part[:, :, :, pl.ds(n * step, step)] = out.reshape(4, 4, 8, step).astype(BF16)

    axes2 = (("x", "z"), ("z", "x"))
    rings = [[], []]

    def start2(i, k):
        first, second = axes2[i]
        j = (at[second] + STEPS[k]) % 4
        ring = ScatterRing(
            copies,
            lambda t, cut: part2[i].at[t, j, :, pl.ds(*cut)],
            land1[i].at[k],
            pass1[i].at[k],
            side(first),
            HALF_CUT,
        )
        ring.start()
        rings[i].append(ring)

    arriving = [[], []]

    def end2(i, k):
        second = axes2[i][1]
        j = (at[second] + STEPS[k]) % 4
        for cut, value in zip(HALF_CUT, rings[i][k].end()):
            next2[i][j, :, pl.ds(*cut)] = value.astype(BF16)
        if k < 3:
            arriving[i].append(
                copies.start(next2[i].at[j], land2[i].at[k], peer_along(second, STEPS[k]))
            )

    project(high, low, part2[0], 0)
    start2(0, 0)
    start2(0, 1)
    project(low, high, part2[1], HALF)
    start2(1, 0)
    start2(1, 1)
    for k in range(4):
        for i in range(2):
            rings[i][k].middle()
            if k < 2:
                start2(i, k + 2)
        if k > 0:
            for i in range(2):
                end2(i, k - 1)
    for i in range(2):
        end2(i, 3)
    across = (r, (g + 16) % 32)
    paired = []
    for i in range(2):
        total = next2[i][at[axes2[i][1]]].astype(F32)
        for k in range(3):
            arriving[i][k].wait_recv()
            total += land2[i][k].astype(F32)
        for j in range(2):
            last2[i][j] = total[4 * j : 4 * j + 4].astype(BF16)
        paired.append(copies.start(last2[i].at[1 - y_lo], landy[i], across))
    squares = jnp.zeros((SEQ, 1), F32)
    kept = []
    for i in range(2):
        paired[i].wait_recv()
        cols = pl.ds(i * HALF, HALF)
        total = last2[i][y_lo].astype(F32) + landy[i][...].astype(F32) + hidden_ref[:, cols].astype(F32)
        resid = total.astype(BF16)
        resid_ref[:, cols] = resid
        resid = resid.astype(F32)
        kept.append(resid)
        squares += jnp.sum(resid * resid, axis=1, keepdims=True)
    factor = lax.rsqrt(squares / D + EPS)
    normed = jnp.concatenate(kept, axis=1) * factor * gain_ref[...].astype(F32)
    normed = normed.astype(BF16)

    short = []
    for p in range(3):
        c = AXES[p][2]
        slots[p][at[c]] = normed[:, STARTS[p] : STARTS[p] + WIDTHS[p]]
        block = slots[p].at[at[c]]
        short.append([copies.start(block, block, peer_along(c, step)) for step in (2, 1, 3)])
    second = []
    for p in range(3):
        a, b, c = AXES[p]
        for copy in short[p]:
            copy.wait_recv()
        for s in range(4):
            blocks[p][pl.ds(4 * s, 4), :] = slots[p][s].astype(F32)
        all_rows[p][at[a], at[b]] = blocks[p][...].astype(BF16)
        ref = all_rows[p].at[at[a]]
        second.append(
            GatherRing(copies, lambda j, cut, ref=ref: ref.at[j, :, pl.ds(*cut)], side(b), CUTS[p])
        )
        second[p].start()
    third = [{}, {}, {}]

    def start3(p, step):
        a, b, c = AXES[p]
        j = (at[b] + step) % 4
        ring = GatherRing(
            copies, lambda t, cut: all_rows[p].at[t, j, :, pl.ds(*cut)], side(a), CUTS[p]
        )
        ring.start()
        third[p][step] = ring

    every = range(3)
    for p in every:
        start3(p, 0)
    for p in every:
        second[p].middle()
    for p in every:
        second[p].near()
        start3(p, 3)
        start3(p, 1)
    for p in every:
        third[p][0].middle()
    for p in every:
        second[p].far()
        start3(p, 2)
    for step in (3, 1, 2):
        for p in every:
            third[p][step].middle()

    row, col = iota((256, 256), 0), iota((256, 256), 1)

    def place(p, i):
        b = i & 3
        of = {"z": (i >> 2) & 3, "y": (i >> 4) & 3, "x": (i >> 6) & 3}
        s, t, u = (of[axis] for axis in AXES[p])
        return ((s * 4 + t) * 4 + u) * 4 + b

    for load in loads[1:]:
        load.wait()
    for copy in traded:
        copy.wait_recv()
    for p in every:
        for step in (0, 3, 1, 2):
            third[p][step].near()
            third[p][step].far()
        rows = all_rows[p][...].reshape(256, WIDTHS[p])
        if p > 0:
            order = jnp.where(col == place(p, row), 1.0, 0.0).astype(BF16)
            rows = jnp.dot(order, rows, preferred_element_type=F32).astype(BF16)
        weights = gates[:, :, pl.ds(STARTS[p], WIDTHS[p])].reshape(4 * FF_OWN, WIDTHS[p])
        product = lax.dot_general(weights, rows, NT, preferred_element_type=F32)
        if p > 0:
            product += sums[...]
        sums[...] = product
    gate, up = sums[pl.ds(0, 2 * FF_OWN), :], sums[pl.ds(2 * FF_OWN, 2 * FF_OWN), :]
    turned[...] = (gate / (1.0 + jnp.exp(-gate)) * up).astype(BF16)

    first = [[], [], []]

    def start1(p, k):
        a, b, c = AXES[p]
        j = (at[b] + STEPS[k]) % 4
        ring = ScatterRing(
            copies,
            lambda t, cut: parts[p].at[t, j, :, pl.ds(*cut)],
            landings[p].at[k],
            passings[p].at[k],
            side(a),
            CUTS[p],
        )
        ring.start()
        first[p].append(ring)

    second = [
        ScatterRing(
            copies,
            lambda t, cut, p=p: nexts[p].at[t, :, pl.ds(*cut)],
            landings2[p],
            passings2[p],
            side(AXES[p][1]),
            CUTS[p],
        )
        for p in every
    ]

    def end1(p, k):
        j = (at[AXES[p][1]] + STEPS[k]) % 4
        for cut, value in zip(CUTS[p], first[p][k].end()):
            nexts[p][j, :, pl.ds(*cut)] = value.astype(BF16)
        if k < 3:
            (second[p].send_far, second[p].send_right, second[p].send_left)[k]()

    for p in every:
        order = jnp.where(row == place(p, col), 1.0, 0.0).astype(BF16)
        act = lax.dot_general(order, turned[...], NT, preferred_element_type=F32).astype(BF16)
        for start, size in CUTS[p]:
            weights = downs[:, :, pl.ds(STARTS[p] + start, size)].reshape(2 * FF_OWN, size)
            out = jnp.dot(act, weights, preferred_element_type=F32)
            parts[p][:, :, :, pl.ds(start, size)] = out.astype(BF16).reshape(4, 4, 16, size)
        start1(p, 0)
        start1(p, 1)
    for k in range(4):
        for p in every:
            first[p][k].middle()
            if k < 2:
                start1(p, k + 2)
        if k > 0:
            for p in every:
                end1(p, k - 1)
    for p in every:
        second[p].middle()
    for p in every:
        end1(p, 3)
    short = []
    for p in every:
        for (start, size), value in zip(CUTS[p], second[p].end()):
            for j in range(4):
                lasts[p][j, :, pl.ds(start, size)] = value[4 * j : 4 * j + 4].astype(BF16)
        c = AXES[p][2]
        short.append(
            [
                copies.start(lasts[p].at[(at[c] + step) % 4], landings3[p].at[k], peer_along(c, step))
                for k, step in enumerate((2, 1, 3))
            ]
        )
    for p in every:
        cols = pl.ds(STARTS[p], WIDTHS[p])
        total = resid_ref[:, cols].astype(F32) + lasts[p][at[AXES[p][2]]].astype(F32)
        for k in range(3):
            short[p][k].wait_recv()
            total += landings3[p][k].astype(F32)
        out_ref[:, cols] = total.astype(BF16)
    copies.finish()


def layer_tail(lat, wuv, w_out, hidden_in, gain, wg_t, wu_t, wd):
    vmem = pl.BlockSpec(memory_space=pltpu.VMEM)
    hbm = pl.BlockSpec(memory_space=pl.ANY)
    half = HALF // 2
    halves = [cut[0][1] for cut in CUTS]
    scratch = [
        pltpu.VMEM((32, 8, KV_RANK), BF16),
        pltpu.VMEM((256, D), BF16),
        pltpu.VMEM((4, FF_OWN, D), BF16),
        pltpu.VMEM((2, FF_OWN, D), BF16),
        pltpu.VMEM((4 * FF_OWN, 256), F32),
        pltpu.VMEM((2 * FF_OWN, 256), BF16),
        pltpu.VMEM((SEQ, D), BF16),
    ]
    for shape in (
        (4, 4, 8, HALF), (4, 8, HALF), (3, 8, HALF), (2, 4, HALF), (4, 6, 8, half), (4, 2, 8, half), (4, HALF),
    ):
        scratch += [pltpu.VMEM(shape, BF16)] * 2
    scratch += [pltpu.VMEM((4, 4, w), BF16) for w in WIDTHS]
    scratch += [pltpu.VMEM((16, w), F32) for w in WIDTHS]
    for lead in ((4, 4, 16), (4, 4, 16), (4, 16), (4, 4)):
        scratch += [pltpu.VMEM((*lead, w), BF16) for w in WIDTHS]
    for lead in ((4, 6, 16), (4, 2, 16), (6, 16), (2, 16)):
        scratch += [pltpu.VMEM((*lead, h), BF16) for h in halves]
    scratch += [pltpu.VMEM((3, 4, w), BF16) for w in WIDTHS]
    count = 31 + 3 + 2 * (24 + 3 + 1) + 3 * (3 + 6 + 24) * 2
    scratch += [pltpu.SemaphoreType.DMA((n,)) for n in (4, count, count)]
    return pl.pallas_call(
        layer_kernel,
        out_shape=jax.ShapeDtypeStruct((SEQ, D), BF16),
        in_specs=[vmem] * 2 + [hbm] + [vmem] * 2 + [hbm] * 3,
        out_specs=vmem,
        scratch_shapes=scratch,
        compiler_params=pltpu.CompilerParams(
            collective_id=1, has_side_effects=True, vmem_limit_bytes=VMEM_LIMIT
        ),
        name="layer_tail",
    )(lat, wuv, w_out, hidden_in, gain, wg_t, wu_t, wd)


def on_device(
    hidden_in, q_nope, q_rope, new_kv, cache_kv, lengths,
    w_uk, w_uv, w_out, norm_gain, w_gate, w_up, w_down,
):
    queries, value_up = spread_queries(q_nope, q_rope.reshape(SEQ, H, ROPE), w_uk, w_uv)
    latent = attend(lengths, queries, new_kv, jnp.swapaxes(cache_kv, 1, 2))
    return layer_tail(
        latent, value_up.reshape(KV_RANK, 256), w_out, hidden_in, norm_gain[None, :], w_gate.T, w_up.T, w_down
    )


def solution(mesh):
    return jax.shard_map(
        on_device,
        mesh=mesh,
        in_specs=(
            P(("rep", "grp"), None),
            P(("rep", "grp"), None),
            P(("rep", "grp"), None),
            P(("rep", "grp"), None),
            P(("rep", "grp"), None, None),
            P(("rep", "grp")),
            P("rep", None),
            P("rep", None),
            P("grp", None),
            P(),
            P(None, ("rep", "grp")),
            P(None, ("rep", "grp")),
            P(("rep", "grp"), None),
        ),
        out_specs=P(("rep", "grp"), None),
        check_vma=False,
    )
```

```python
import functools

import jax
import jax.numpy as jnp
from jax import lax
from jax.experimental import pallas as pl
from jax.experimental.pallas import tpu as pltpu
from jax.sharding import PartitionSpec as P

D = 7168
FF_OWN = 144
H = 64
NOPE = 128
ROPE = 64
VH = 128
KV_RANK = 512
CACHE = 4096
SEQ = 4
NB = SEQ
BLOCK = 1024
DIRECT_GATHER = (2,)
DIRECT_SCATTER = (2, 3)
DIRECT_PROJECT = (2, 3)
LAG = 1
RINGS = 4 - len(DIRECT_SCATTER)
RINGS_PROJECT = 4 - len(DIRECT_PROJECT)
START_AHEAD = 2
EPS = 1e-06
SCALE = float(NOPE + ROPE) ** (-0.5)
MESH = pl.DeviceIdType.MESH
F32 = jnp.float32
BF16 = jnp.bfloat16
NT = (((1,), (1,)), ((), ()))
VMEM_LIMIT = 67043328


def coordinates():
    r, g = lax.axis_index("rep"), lax.axis_index("grp")
    return dict(
        r=r, g=g, core=r % 2, y=(r // 2) * 2 + g // 16, x=(g // 4) % 4, z=g % 4
    )


def device_at(at, **moved):
    x, y, z = (moved.get(k, at[k]) for k in "xyz")
    return ((y // 2) * 2 + at["core"], ((y % 2) * 4 + x) * 4 + z)


class Copies:
    def __init__(self, send_sems, recv_sems):
        self.send, self.recv, self.used, self.all = send_sems, recv_sems, 0, []

    def start(self, src, dst, device):
        k = self.used
        self.used += 1
        copy = pltpu.make_async_remote_copy(
            src_ref=src,
            dst_ref=dst,
            send_sem=self.send.at[k],
            recv_sem=self.recv.at[k],
            device_id=device,
            device_id_type=MESH,
        )
        copy.start()
        self.all.append(copy)
        return copy

    def finish(self):
        for copy in self.all:
            copy.wait_send()


def barrier_with(peers):
    sem = pltpu.get_barrier_semaphore()
    for peer in peers:
        pl.semaphore_signal(sem, inc=1, device_id=peer, device_id_type=MESH)
    pl.semaphore_wait(sem, len(peers))


class GatherRing:
    def __init__(self, copies, block, side, cut):
        self.copies, self.block, self.cut = copies, block, cut
        self.me, self.left, self.right = side

    def go(self, j, half, device):
        ref = self.block(j, self.cut[half])
        return self.copies.start(ref, ref, device)

    def start(self):
        m = self.me
        self.ra = self.go(m, 0, self.right)
        self.lb = self.go(m, 1, self.left)
        self.rb = self.go(m, 1, self.right)
        self.la = self.go(m, 0, self.left)

    def middle(self):
        m = self.me
        self.ra.wait_recv()
        self.rf = self.go((m + 3) % 4, 0, self.right)
        self.lb.wait_recv()
        self.lf = self.go((m + 1) % 4, 1, self.left)

    def near(self):
        self.rb.wait_recv()
        self.la.wait_recv()

    def far(self):
        self.rf.wait_recv()
        self.lf.wait_recv()


class ScatterRing:
    def __init__(self, copies, chunk, landing, passing, side, cut):
        self.copies, self.chunk, self.landing, self.passing, self.cut = copies, chunk, landing, passing, cut
        self.me, self.left, self.right = side

    def part(self, step, half):
        return self.chunk((self.me + step) % 4, self.cut[half])

    def land(self, k, half):
        return self.landing.at[k, :, pl.ds(0, self.cut[half][1])]

    def send_far(self):
        go = self.copies.start
        self.r0 = go(self.part(2, 0), self.land(0, 0), self.right)
        self.l0 = go(self.part(2, 1), self.land(1, 1), self.left)

    def send_right(self):
        self.r1 = self.copies.start(self.part(1, 1), self.land(2, 1), self.right)

    def send_left(self):
        self.l1 = self.copies.start(self.part(3, 0), self.land(3, 0), self.left)

    def start(self):
        self.send_far()
        self.send_right()
        self.send_left()

    def value(self, ref):
        return ref[...].astype(F32)

    def pass_on(self, copy, step, half, device):
        copy.wait_recv()
        held = self.passing.at[half, :, pl.ds(0, self.cut[half][1])]
        held[...] = self.part(step, half)[...] + self.land(half, half)[...]
        return self.copies.start(held, self.land(4 + half, half), device)

    def middle(self):
        self.r2 = self.pass_on(self.r0, 1, 0, self.right)
        self.l2 = self.pass_on(self.l0, 3, 1, self.left)

    def end(self):
        self.l1.wait_recv()
        self.r2.wait_recv()
        first = self.value(self.part(0, 0)) + self.value(self.land(4, 0)) + self.value(self.land(3, 0))
        self.r1.wait_recv()
        self.l2.wait_recv()
        second = self.value(self.part(0, 1)) + self.value(self.land(2, 1)) + self.value(self.land(5, 1))
        return first, second


class GatherDirect:
    def __init__(self, copies, block, me, devices):
        self.copies, self.block, self.me, self.devices = copies, block, me, devices

    def start(self):
        ref = self.block(self.me)
        self.sent = [self.copies.start(ref, ref, device) for device in self.devices]

    def middle(self):
        pass

    def near(self):
        pass

    def far(self):
        for copy in self.sent:
            copy.wait_recv()


class ScatterDirect:
    def __init__(self, copies, chunk, landing, me, devices, cut):
        self.copies, self.chunk, self.landing, self.me = copies, chunk, landing, me
        self.devices, self.cut = devices, cut

    def start(self):
        width = sum(size for _, size in self.cut)
        self.sent = [
            self.copies.start(
                self.chunk((self.me + step) % 4, (0, width)), self.landing.at[i, :, pl.ds(0, width)], device
            )
            for i, (step, device) in enumerate(zip((2, 1, 3), self.devices))
        ]

    def middle(self):
        pass

    def end(self):
        for copy in self.sent:
            copy.wait_recv()
        values = []
        for start, size in self.cut:
            value = self.chunk(self.me, (start, size))[...].astype(F32)
            for i in range(3):
                value += self.landing[i, :, pl.ds(start, size)].astype(F32)
            values.append(value)
        return values


GROUP = 16
HALF = D // 2
HALF_CUT = ((0, HALF // 2), (HALF // 2, HALF // 2))
WIDTHS = (2432, 2432, 2304)
STARTS = (0, 2432, 4864)
CUTS = tuple(
    ((0, (w // 256) * 128 + (w % 256)), ((w // 256) * 128 + (w % 256), (w // 256) * 128)) for w in WIDTHS
)
AXES = (("x", "y", "z"), ("y", "z", "x"), ("z", "x", "y"))
AXES2 = (("x", "z"), ("z", "x"))
STEPS = (2, 1, 3, 0)
LB = NB.bit_length() - 1


def iota(shape, dim):
    return lax.broadcasted_iota(jnp.int32, shape, dim)


class Named:
    def __init__(self):
        self.names, self.shapes = [], []

    def add(self, name, *shapes):
        self.names.append((name, len(shapes)))
        self.shapes += shapes

    def bind(self, refs):
        refs = list(refs)
        for name, count in self.names:
            taken, refs = refs[:count], refs[count:]
            setattr(self, name, taken[0] if count == 1 else taken)
        return self


def declare():
    s = Named()
    half = HALF // 2
    halves = [cut[0][1] for cut in CUTS]
    b16 = lambda *shape: pltpu.VMEM(shape, BF16)
    f32 = lambda *shape: pltpu.VMEM(shape, F32)
    s.add("gathered", b16(4, SEQ, H * NOPE))
    s.add("rows", f32(16, GROUP * NOPE))
    s.add("wuk", b16(128, H * NOPE))
    s.add("tall", f32(16, GROUP, NOPE))
    s.add("made", b16(4, SEQ, H, NOPE))
    s.add("queries", b16(SEQ, H, KV_RANK + ROPE))
    s.add("wuv", b16(4, 128, 256))
    s.add("cache", b16(SEQ, KV_RANK + ROPE, CACHE))
    s.add("scores", f32(SEQ, H, CACHE))
    s.add("lanes", f32(KV_RANK // 128, H, 128))
    s.add("mixed", f32(KV_RANK // 128, H // 2, NB, 128))
    s.add("wout", b16(256, D))
    s.add("gates", b16(4, FF_OWN, D))
    s.add("downs", b16(2, FF_OWN, D))
    s.add("sums", f32(4 * FF_OWN, 64 * NB))
    s.add("turned", b16(2 * FF_OWN, 64 * NB))
    s.add("blocks", *[f32(4 * NB, w) for w in WIDTHS])
    s.add("gain", f32(1, D))
    s.add("rope", f32(SEQ, H, 128))
    for f in range(1):
        s.add(f"lat{f}", b16(H // 2, 2, NB, KV_RANK))
        s.add(f"got{f}", b16(H // 2, 2, NB, KV_RANK))
        s.add(f"resid{f}", f32(NB, D))
        for name, shape in (
            ("part2", (4, 4, 2 * NB, HALF)),
            ("next2", (4, 2, NB, HALF)),
            ("land2", (7, NB, HALF)),
            ("land1", (RINGS_PROJECT, 6, 2 * NB, half)),
            ("pass1", (RINGS_PROJECT, 2, 2 * NB, half)),
            ("whole1", (4 - RINGS_PROJECT, 3, 2 * NB, HALF)),
        ):
            s.add(f"{name}{f}", *[b16(*shape)] * 2)
        for name, lead in (
            ("slots", (4, 4, NB)),
            ("all_rows", (4, 4, 4 * NB)),
            ("parts", (4, 4, 4 * NB)),
            ("lasts", (4, 4, NB)),
            ("landings3", (15, NB)),
            ("wholes", (4 - RINGS, 3, 4 * NB)),
        ):
            s.add(f"{name}{f}", *[b16(*lead, w) for w in WIDTHS])
        for name, lead in (
            ("landings", (RINGS, 6, 4 * NB)),
            ("passings", (RINGS, 2, 4 * NB)),
        ):
            s.add(f"{name}{f}", *[b16(*lead, h) for h in halves])
    count = 6 + 6 * (H // GROUP) + 62 + 2 * (24 + 7) + 3 * (15 + 24) * 2
    s.add("local_sems", pltpu.SemaphoreType.DMA((5,)))
    s.add("wuk_sems", pltpu.SemaphoreType.DMA((H // GROUP,)))
    s.add("cache_sems", pltpu.SemaphoreType.DMA((SEQ,)))
    s.add("send_sems", pltpu.SemaphoreType.DMA((count,)))
    s.add("recv_sems", pltpu.SemaphoreType.DMA((count,)))
    return s


def layer_kernel(
    len_ref, q_ref, rope_ref, new_ref, hidden_ref, gain_ref,
    cache_hbm, wuk_hbm, wuv_hbm, wout_hbm, wg_hbm, wu_hbm, wd_hbm, out_ref, *refs,
):
    s = declare().bind(refs)
    at = coordinates()
    r, g = at["r"], at["g"]
    y_lo = g // 16
    copies = Copies(s.send_sems, s.recv_sems)
    every = range(3)

    def peer_along(axis, step):
        return device_at(at, **{axis: (at[axis] + step) % 4})

    def side(axis):
        return at[axis], peer_along(axis, 3), peer_along(axis, 1)

    def three(axis):
        return [peer_along(axis, step) for step in (2, 1, 3)]

    wide = GROUP * NOPE
    spans = [pl.ds(i * wide, wide) for i in range(H // GROUP)]
    wuk_loads = [
        pltpu.make_async_copy(wuk_hbm.at[:, span], s.wuk.at[:, span], s.wuk_sems.at[i])
        for i, span in enumerate(spans)
    ]
    mine = wuv_hbm.at[:, pl.ds(pl.multiple_of(g * 256, 256), 256)]
    own_wuv = pltpu.make_async_copy(mine, s.wuv.at[r], s.local_sems.at[4])
    cache_loads = [
        pltpu.make_async_copy(cache_hbm.at[b], s.cache.at[b], s.cache_sems.at[b]) for b in range(SEQ)
    ]
    loads = [
        pltpu.make_async_copy(src, dst, s.local_sems.at[i])
        for i, (src, dst) in enumerate(
            ((wout_hbm, s.wout), (wg_hbm, s.gates.at[0]), (wu_hbm, s.gates.at[2]), (wd_hbm, s.downs.at[0]))
        )
    ]
    for load in wuk_loads + [own_wuv] + cache_loads + loads:
        load.start()

    twin = (r + 1 - 2 * at["core"], g)
    other = (r + 2) % 4
    cousins = [((r + k) % 4, g) for k in (1, 2, 3)]
    peers = [(r, (g + k) % 32) for k in range(1, 32)]
    across = (r, (g + 16) % 32)
    far_y = [
        device_at(at, **{axis: (at[axis] + k) % 4, "y": 2 * (1 - at["y"] // 2) + j})
        for axis in "xz"
        for k in range(4)
        for j in range(2)
        if axis == "x" or k > 0
    ]
    near_y = [(r + 1 - 2 * at["core"], g), (other + 1 - 2 * at["core"], g)]
    barrier_with(peers + near_y + far_y)

    incoming = [
        [copies.start(q_ref.at[:, span], s.gathered.at[r, :, span], peer) for peer in cousins]
        for span in spans
    ]
    s.gathered[r] = q_ref[...]
    for k in range(H // 2):
        pair = rope_ref[:, pl.ds(k * 128, 128)].astype(F32)
        s.rope[:, 2 * k, :] = pair
        s.rope[:, 2 * k + 1, :] = pltpu.roll(pair, 64, 1)
    s.queries[:, :, pl.ds(KV_RANK, ROPE)] = s.rope[:, :, pl.ds(0, ROPE)].astype(BF16)
    gain = gain_ref[...].astype(F32)
    for k in range(D // 128):
        s.gain[:, pl.ds(k * 128, 128)] = gain[k : k + 1]
    slice_of_rank = pl.ds(pl.multiple_of(r * NOPE, NOPE), NOPE)
    new_rows = new_ref[...].astype(F32)

    def rotary_scores(b):
        length = len_ref[b]
        q = s.rope[b, :, pl.ds(0, ROPE)].astype(BF16)
        lane = iota((H, BLOCK), 1)
        cache_loads[b].wait()
        for c in range(CACHE // BLOCK):
            cols = pl.ds(c * BLOCK, BLOCK)
            v = jnp.dot(q, s.cache[b, pl.ds(KV_RANK, ROPE), cols], preferred_element_type=F32) * SCALE
            s.scores[b, :, cols] = jnp.where(lane < length - c * BLOCK, v, -jnp.inf)

    rotary_scores(0)
    rotary_scores(1)
    back = []
    for i, span in enumerate(spans):
        for copy in incoming[i]:
            copy.wait_recv()
        wuk_loads[i].wait()
        for m in range(4):
            s.rows[pl.ds(4 * m, 4), :] = s.gathered[m, :, span].astype(F32)
        for k in range(GROUP):
            s.tall[:, k, :] = lax.dot_general(
                s.rows[:, pl.ds(k * NOPE, NOPE)].astype(BF16),
                s.wuk[:, pl.ds((i * GROUP + k) * NOPE, NOPE)],
                NT,
                preferred_element_type=F32,
            )
        heads = pl.ds(i * GROUP, GROUP)
        s.made[:, :, heads, :] = s.tall[...].astype(BF16).reshape(4, SEQ, GROUP, NOPE)
        for peer in cousins:
            back.append(
                copies.start(s.made.at[peer[0], :, heads, :], s.queries.at[:, heads, slice_of_rank], peer)
            )
    weights = [copies.start(mine, s.wuv.at[r], peer) for peer in cousins]
    traded = [
        copies.start(src, dst, twin)
        for src, dst in ((wg_hbm, s.gates.at[1]), (wu_hbm, s.gates.at[3]), (wd_hbm, s.downs.at[1]))
    ]
    s.queries[:, :, slice_of_rank] = s.made[r]
    rotary_scores(2)
    rotary_scores(3)
    for copy in back:
        copy.wait_recv()

    def attend(b, local):
        q = s.queries[b]
        new = new_rows[b : b + 1]
        own = jnp.sum(q.astype(F32) * new, axis=1, keepdims=True) * SCALE
        q = q[:, :KV_RANK]
        top = jnp.full((H, 128), -jnp.inf, F32)
        for c in range(CACHE // BLOCK):
            cols = pl.ds(c * BLOCK, BLOCK)
            v = jnp.dot(q, s.cache[b, pl.ds(0, KV_RANK), cols], preferred_element_type=F32) * SCALE
            v += s.scores[b, :, cols]
            s.scores[b, :, cols] = v
            for i in range(BLOCK // 128):
                top = jnp.maximum(top, v[:, i * 128 : (i + 1) * 128])
        top = jnp.maximum(jnp.max(top, axis=1, keepdims=True), own)
        own = jnp.exp(own - top)
        total = jnp.zeros((H, 128), F32)
        mix = own * new[:, :KV_RANK]
        for c in range(CACHE // BLOCK):
            cols = pl.ds(c * BLOCK, BLOCK)
            p = jnp.exp(s.scores[b, :, cols] - top)
            for i in range(BLOCK // 128):
                total += p[:, i * 128 : (i + 1) * 128]
            mix += lax.dot_general(
                p.astype(BF16), s.cache[b, pl.ds(0, KV_RANK), cols], NT, preferred_element_type=F32
            )
        mix = mix / (jnp.sum(total, axis=1, keepdims=True) + own)
        for t in range(KV_RANK // 128):
            s.lanes[t] = mix[:, t * 128 : (t + 1) * 128]
            for h in range(2):
                s.mixed[t, :, 2 * local + h, :] = s.lanes[t, pl.ds(h, H // 2, stride=2), :]

    def place(p, i):
        b = i & (NB - 1)
        of = {"z": (i >> LB) & 3, "y": (i >> (LB + 2)) & 3, "x": (i >> (LB + 4)) & 3}
        t, u, v = (of[axis] for axis in AXES[p])
        return ((t * 4 + u) * 4 + v) * NB + b

    lat, got = s.lat0, s.got0

    def send_latents(pair):
        for t in range(KV_RANK // 128):
            lat[:, pair, :, pl.ds(t * 128, 128)] = s.mixed[t].astype(BF16)
        return [copies.start(lat.at[peer[1], pair], got.at[g, pair], peer) for peer in peers]

    def flow(f):
        buf = lambda name: getattr(s, f"{name}{f}")
        arriving = send_latents(1)
        got[g] = lat[g]
        yield
        for copy in early + arriving:
            copy.wait_recv()
        if f == 0:
            for copy in weights:
                copy.wait_recv()
            own_wuv.wait()
            loads[0].wait()
        rows_in = got[...].reshape(64 * NB, KV_RANK)
        heads = jnp.dot(rows_in, s.wuv[...].reshape(KV_RANK, 256), preferred_element_type=F32)
        row, col = iota((64 * NB, 256), 0), iota((64 * NB, 256), 1)
        heads = jnp.where((row & 1) == (col >> 7), heads, 0.0).astype(BF16)
        row, col = iota((32 * NB, 64 * NB), 0), iota((32 * NB, 64 * NB), 1)
        b, y_of, low, high = row & (NB - 1), (row >> LB) & 1, (row >> (LB + 1)) & 3, row >> (LB + 3)
        part2, next2, land2 = buf("part2"), buf("next2"), buf("land2")
        rings = [[], []]
        gathering = [[], []]

        def project(x_of, z_of, part, first_col):
            source = (((y_of * 4 + x_of) * 4) + z_of) * NB + b
            pick = jnp.where((col >> 1) == source, 1.0, 0.0).astype(BF16)
            rows = jnp.dot(pick, heads, preferred_element_type=F32).astype(BF16)
            step = HALF // 4
            for n in range(4):
                out = jnp.dot(
                    rows, s.wout[:, pl.ds(first_col + n * step, step)], preferred_element_type=F32
                )
                part[:, :, :, pl.ds(n * step, step)] = out.reshape(4, 4, 2 * NB, step).astype(BF16)

        def start2(i, k):
            j = (at[AXES2[i][1]] + STEPS[k]) % 4
            first = AXES2[i][0]
            chunk = lambda t, cut: part2[i].at[t, j, :, pl.ds(*cut)]
            if k in DIRECT_PROJECT:
                ring = ScatterDirect(copies, chunk, buf("whole1")[i].at[k - RINGS_PROJECT], at[first], three(first), HALF_CUT)
            else:
                ring = ScatterRing(
                    copies, chunk, buf("land1")[i].at[k], buf("pass1")[i].at[k], side(first), HALF_CUT
                )
            ring.start()
            rings[i].append(ring)

        def end2(i, k):
            second = AXES2[i][1]
            j = (at[second] + STEPS[k]) % 4
            for cut, value in zip(HALF_CUT, rings[i][k].end()):
                for half in range(2):
                    next2[i][j, half, :, pl.ds(*cut)] = value[NB * half : NB * half + NB].astype(BF16)
            for step in (1, 0):
                if k < 3 or step > 0:
                    to = (y_lo + step) % 2
                    device = device_at(at, **{second: j, "y": at["y"] - y_lo + to})
                    landing = land2[i].at[len(gathering[i])]
                    gathering[i].append(copies.start(next2[i].at[j, to], landing, device))

        project(high, low, part2[0], 0)
        start2(0, 0)
        start2(0, 1)
        project(low, high, part2[1], HALF)
        start2(1, 0)
        start2(1, 1)
        for k in range(4):
            yield
            for i in range(2):
                rings[i][k].middle()
                if k < 2:
                    start2(i, k + 2)
            if k >= LAG:
                for i in range(2):
                    end2(i, k - LAG)
        for k in range(4 - LAG, 4):
            yield
            for i in range(2):
                end2(i, k)
        yield
        squares = jnp.zeros((NB, 1), F32)
        kept = []
        for i in range(2):
            cols = pl.ds(i * HALF, HALF)
            total = next2[i][at[AXES2[i][1]], y_lo].astype(F32) + hidden_ref[:, cols].astype(F32)
            for k in range(7):
                gathering[i][k].wait_recv()
                total += land2[i][k].astype(F32)
            resid = total.astype(BF16).astype(F32)
            buf("resid")[:, cols] = resid
            kept.append(resid)
            squares += jnp.sum(resid * resid, axis=1, keepdims=True)
        factor = lax.rsqrt(squares / D + EPS)
        normed = jnp.concatenate(kept, axis=1) * factor * s.gain[...]
        normed = normed.astype(BF16)

        slots, all_rows = buf("slots"), buf("all_rows")
        plane = [{}, {}, {}]
        for p in every:
            _, second, last = AXES[p]
            slots[p][at[second], at[last]] = normed[:, STARTS[p] : STARTS[p] + WIDTHS[p]]
        for step in (0, 1, 3, 2):
            for p in every:
                _, second, last = AXES[p]
                block = slots[p].at[at[second], at[last]]
                plane[p][step] = [
                    copies.start(
                        block,
                        block,
                        device_at(at, **{second: (at[second] + step) % 4, last: (at[last] + k) % 4}),
                    )
                    for k in (1, 3, 2, 0)
                    if step > 0 or k > 0
                ]
        yield
        third = [{}, {}, {}]

        def start3(p, step):
            first, second, _ = AXES[p]
            j = (at[second] + step) % 4
            for copy in plane[p][(4 - step) % 4]:
                copy.wait_recv()
            for m in range(4):
                s.blocks[p][pl.ds(NB * m, NB), :] = slots[p][j, m].astype(F32)
            all_rows[p][at[first], j] = s.blocks[p][...].astype(BF16)
            if step in DIRECT_GATHER:
                ring = GatherDirect(copies, lambda t: all_rows[p].at[t, j], at[first], three(first))
            else:
                ring = GatherRing(
                    copies, lambda t, cut: all_rows[p].at[t, j, :, pl.ds(*cut)], side(first), CUTS[p]
                )
            ring.start()
            third[p][step] = ring

        for step in (0, 3, 1, 2):
            for p in every:
                start3(p, step)
            if step == 1:
                for p in every:
                    third[p][0].middle()
        for step in (3, 1, 2):
            for p in every:
                third[p][step].middle()
        yield
        if f == 0:
            for load in loads[1:]:
                load.wait()
            for copy in traded:
                copy.wait_recv()
        row, col = iota((64 * NB, 64 * NB), 0), iota((64 * NB, 64 * NB), 1)
        for p in every:
            for step in (0, 3, 1, 2):
                third[p][step].near()
                third[p][step].far()
            rows = all_rows[p][...].reshape(64 * NB, WIDTHS[p])
            if p > 0:
                order = jnp.where(col == place(p, row), 1.0, 0.0).astype(BF16)
                rows = jnp.dot(order, rows, preferred_element_type=F32).astype(BF16)
            matrix = s.gates[:, :, pl.ds(STARTS[p], WIDTHS[p])].reshape(4 * FF_OWN, WIDTHS[p])
            product = lax.dot_general(matrix, rows, NT, preferred_element_type=F32)
            if p > 0:
                product += s.sums[...]
            s.sums[...] = product
        gate, up = s.sums[pl.ds(0, 2 * FF_OWN), :], s.sums[pl.ds(2 * FF_OWN, 2 * FF_OWN), :]
        s.turned[...] = (gate / (1.0 + jnp.exp(-gate)) * up).astype(BF16)

        parts, lasts = buf("parts"), buf("lasts")
        first = [[], [], []]

        def start1(p, k):
            j = (at[AXES[p][1]] + STEPS[k]) % 4
            axis = AXES[p][0]
            chunk = lambda t, cut: parts[p].at[k, t, :, pl.ds(*cut)]
            if k in DIRECT_SCATTER:
                ring = ScatterDirect(copies, chunk, buf("wholes")[p].at[k - RINGS], at[axis], three(axis), CUTS[p])
            else:
                ring = ScatterRing(
                    copies, chunk, buf("landings")[p].at[k], buf("passings")[p].at[k], side(axis), CUTS[p]
                )
            ring.start()
            first[p].append(ring)

        ending = [[], [], []]

        def end1(p, k):
            _, second, last = AXES[p]
            j = (at[second] + STEPS[k]) % 4
            for (start, size), value in zip(CUTS[p], first[p][k].end()):
                for m in range(4):
                    lasts[p][j, m, :, pl.ds(start, size)] = value[NB * m : NB * m + NB].astype(BF16)
            for step in (2, 1, 3, 0):
                if k < 3 or step > 0:
                    to = (at[last] + step) % 4
                    device = device_at(at, **{second: j, last: to})
                    landing = buf("landings3")[p].at[len(ending[p])]
                    ending[p].append(copies.start(lasts[p].at[j, to], landing, device))

        acts = []
        for p in every:
            k = row >> (LB + 4)
            step = jnp.where(k == 0, 2, jnp.where(k == 1, 1, jnp.where(k == 2, 3, 0)))
            lead = (row >> (LB + 2)) & 3
            middle = (step + at[AXES[p][1]]) & 3
            index = (lead * 4 + middle) * (4 * NB) + (row & (4 * NB - 1))
            order = jnp.where(index == place(p, col), 1.0, 0.0).astype(BF16)
            acts.append(lax.dot_general(order, s.turned[...], NT, preferred_element_type=F32).astype(BF16))
        for k in range(4):
            for p in every:
                for start, size in CUTS[p]:
                    matrix = s.downs[:, :, pl.ds(STARTS[p] + start, size)].reshape(2 * FF_OWN, size)
                    out = jnp.dot(
                        acts[p][16 * NB * k : 16 * NB * (k + 1)], matrix, preferred_element_type=F32
                    )
                    parts[p][k, :, :, pl.ds(start, size)] = out.reshape(4, 4 * NB, size).astype(BF16)
                if k < START_AHEAD:
                    start1(p, k)
        for k in range(4):
            yield
            for p in every:
                first[p][k].middle()
                if k + START_AHEAD < 4:
                    start1(p, k + START_AHEAD)
            if k >= LAG:
                for p in every:
                    end1(p, k - LAG)
        for k in range(4 - LAG, 4):
            yield
            for p in every:
                end1(p, k)
        yield
        for p in every:
            _, second, last = AXES[p]
            cols = pl.ds(STARTS[p], WIDTHS[p])
            total = buf("resid")[:, cols] + lasts[p][at[second], at[last]].astype(F32)
            for k in range(15):
                ending[p][k].wait_recv()
                total += buf("landings3")[p][k].astype(F32)
            out_ref[:, cols] = total.astype(BF16)
        yield

    early = []
    for b in range(SEQ):
        attend(b, b % 2)
        if b == 1:
            early = send_latents(0)
    for _ in flow(0):
        pass
    copies.finish()


def on_device(
    hidden_in, q_nope, q_rope, new_kv, cache_kv, lengths,
    w_uk, w_uv, w_out, norm_gain, w_gate, w_up, w_down,
):
    vmem = pl.BlockSpec(memory_space=pltpu.VMEM)
    hbm = pl.BlockSpec(memory_space=pl.ANY)
    return pl.pallas_call(
        layer_kernel,
        out_shape=jax.ShapeDtypeStruct((SEQ, D), BF16),
        in_specs=[pl.BlockSpec(memory_space=pltpu.SMEM)] + [vmem] * 5 + [hbm] * 7,
        out_specs=vmem,
        scratch_shapes=declare().shapes,
        compiler_params=pltpu.CompilerParams(
            collective_id=0, has_side_effects=True, vmem_limit_bytes=VMEM_LIMIT
        ),
        name="layer",
    )(
        lengths, q_nope, q_rope, new_kv, hidden_in, norm_gain.reshape(D // 128, 128),
        jnp.swapaxes(cache_kv, 1, 2), w_uk, w_uv, w_out, w_gate.T, w_up.T, w_down,
    )


def solution(mesh):
    return jax.shard_map(
        on_device,
        mesh=mesh,
        in_specs=(
            P(("rep", "grp"), None),
            P(("rep", "grp"), None),
            P(("rep", "grp"), None),
            P(("rep", "grp"), None),
            P(("rep", "grp"), None, None),
            P(("rep", "grp")),
            P("rep", None),
            P("rep", None),
            P("grp", None),
            P(),
            P(None, ("rep", "grp")),
            P(None, ("rep", "grp")),
            P(("rep", "grp"), None),
        ),
        out_specs=P(("rep", "grp"), None),
        check_vma=False,
    )
```

```python
import functools

import jax
import jax.numpy as jnp
from jax import lax
from jax.experimental import pallas as pl
from jax.experimental.pallas import tpu as pltpu
from jax.sharding import PartitionSpec as P

D = 7168
FF_OWN = 144
H = 64
NOPE = 128
ROPE = 64
VH = 128
KV_RANK = 512
CACHE = 4096
SEQ = 4
NB = SEQ
BLOCK = 1024
DIRECT_GATHER = (2,)
DIRECT_SCATTER = (2, 3)
DIRECT_PROJECT = (2, 3)
LAG = 1
RINGS = 4 - len(DIRECT_SCATTER)
RINGS_PROJECT = 4 - len(DIRECT_PROJECT)
START_AHEAD = 2
EPS = 1e-06
SCALE = float(NOPE + ROPE) ** (-0.5)
MESH = pl.DeviceIdType.MESH
F32 = jnp.float32
BF16 = jnp.bfloat16
NT = (((1,), (1,)), ((), ()))
VMEM_LIMIT = 67043328


def coordinates():
    r, g = lax.axis_index("rep"), lax.axis_index("grp")
    return dict(
        r=r, g=g, core=r % 2, y=(r // 2) * 2 + g // 16, x=(g // 4) % 4, z=g % 4
    )


def device_at(at, **moved):
    x, y, z = (moved.get(k, at[k]) for k in "xyz")
    return ((y // 2) * 2 + at["core"], ((y % 2) * 4 + x) * 4 + z)


class Copies:
    def __init__(self, send_sems, recv_sems):
        self.send, self.recv, self.used, self.all = send_sems, recv_sems, 0, []

    def start(self, src, dst, device):
        k = self.used
        self.used += 1
        copy = pltpu.make_async_remote_copy(
            src_ref=src,
            dst_ref=dst,
            send_sem=self.send.at[k],
            recv_sem=self.recv.at[k],
            device_id=device,
            device_id_type=MESH,
        )
        copy.start()
        self.all.append(copy)
        return copy

    def finish(self):
        for copy in self.all:
            copy.wait_send()


def barrier_with(peers):
    sem = pltpu.get_barrier_semaphore()
    for peer in peers:
        pl.semaphore_signal(sem, inc=1, device_id=peer, device_id_type=MESH)
    pl.semaphore_wait(sem, len(peers))


class GatherRing:
    def __init__(self, copies, block, side, cut):
        self.copies, self.block, self.cut = copies, block, cut
        self.me, self.left, self.right = side

    def go(self, j, half, device):
        ref = self.block(j, self.cut[half])
        return self.copies.start(ref, ref, device)

    def start(self):
        m = self.me
        self.ra = self.go(m, 0, self.right)
        self.lb = self.go(m, 1, self.left)
        self.rb = self.go(m, 1, self.right)
        self.la = self.go(m, 0, self.left)

    def middle(self):
        m = self.me
        self.ra.wait_recv()
        self.rf = self.go((m + 3) % 4, 0, self.right)
        self.lb.wait_recv()
        self.lf = self.go((m + 1) % 4, 1, self.left)

    def near(self):
        self.rb.wait_recv()
        self.la.wait_recv()

    def far(self):
        self.rf.wait_recv()
        self.lf.wait_recv()


class ScatterRing:
    def __init__(self, copies, chunk, landing, passing, side, cut):
        self.copies, self.chunk, self.landing, self.passing, self.cut = copies, chunk, landing, passing, cut
        self.me, self.left, self.right = side

    def part(self, step, half):
        return self.chunk((self.me + step) % 4, self.cut[half])

    def land(self, k, half):
        return self.landing.at[k, :, pl.ds(0, self.cut[half][1])]

    def send_far(self):
        go = self.copies.start
        self.r0 = go(self.part(2, 0), self.land(0, 0), self.right)
        self.l0 = go(self.part(2, 1), self.land(1, 1), self.left)

    def send_right(self):
        self.r1 = self.copies.start(self.part(1, 1), self.land(2, 1), self.right)

    def send_left(self):
        self.l1 = self.copies.start(self.part(3, 0), self.land(3, 0), self.left)

    def start(self):
        self.send_far()
        self.send_right()
        self.send_left()

    def value(self, ref):
        return ref[...].astype(F32)

    def pass_on(self, copy, step, half, device):
        copy.wait_recv()
        held = self.passing.at[half, :, pl.ds(0, self.cut[half][1])]
        held[...] = self.part(step, half)[...] + self.land(half, half)[...]
        return self.copies.start(held, self.land(4 + half, half), device)

    def middle(self):
        self.r2 = self.pass_on(self.r0, 1, 0, self.right)
        self.l2 = self.pass_on(self.l0, 3, 1, self.left)

    def end(self):
        self.l1.wait_recv()
        self.r2.wait_recv()
        first = self.value(self.part(0, 0)) + self.value(self.land(4, 0)) + self.value(self.land(3, 0))
        self.r1.wait_recv()
        self.l2.wait_recv()
        second = self.value(self.part(0, 1)) + self.value(self.land(2, 1)) + self.value(self.land(5, 1))
        return first, second


class GatherDirect:
    def __init__(self, copies, block, me, devices):
        self.copies, self.block, self.me, self.devices = copies, block, me, devices

    def start(self):
        ref = self.block(self.me)
        self.sent = [self.copies.start(ref, ref, device) for device in self.devices]

    def middle(self):
        pass

    def near(self):
        pass

    def far(self):
        for copy in self.sent:
            copy.wait_recv()


class ScatterDirect:
    def __init__(self, copies, chunk, landing, me, devices, cut):
        self.copies, self.chunk, self.landing, self.me = copies, chunk, landing, me
        self.devices, self.cut = devices, cut

    def start(self):
        width = sum(size for _, size in self.cut)
        self.sent = [
            self.copies.start(
                self.chunk((self.me + step) % 4, (0, width)), self.landing.at[i, :, pl.ds(0, width)], device
            )
            for i, (step, device) in enumerate(zip((2, 1, 3), self.devices))
        ]

    def middle(self):
        pass

    def end(self):
        for copy in self.sent:
            copy.wait_recv()
        values = []
        for start, size in self.cut:
            value = self.chunk(self.me, (start, size))[...].astype(F32)
            for i in range(3):
                value += self.landing[i, :, pl.ds(start, size)].astype(F32)
            values.append(value)
        return values


GROUP = 16
HALF = D // 2
HALF_CUT = ((0, HALF // 2), (HALF // 2, HALF // 2))
WIDTHS = (2432, 2432, 2304)
STARTS = (0, 2432, 4864)
CUTS = tuple(
    ((0, (w // 256) * 128 + (w % 256)), ((w // 256) * 128 + (w % 256), (w // 256) * 128)) for w in WIDTHS
)
AXES = (("x", "y", "z"), ("y", "z", "x"), ("z", "x", "y"))
AXES2 = (("x", "z"), ("z", "x"))
STEPS = (2, 1, 3, 0)
LB = NB.bit_length() - 1


def iota(shape, dim):
    return lax.broadcasted_iota(jnp.int32, shape, dim)


class Named:
    def __init__(self):
        self.names, self.shapes = [], []

    def add(self, name, *shapes):
        self.names.append((name, len(shapes)))
        self.shapes += shapes

    def bind(self, refs):
        refs = list(refs)
        for name, count in self.names:
            taken, refs = refs[:count], refs[count:]
            setattr(self, name, taken[0] if count == 1 else taken)
        return self


def declare():
    s = Named()
    half = HALF // 2
    halves = [cut[0][1] for cut in CUTS]
    b16 = lambda *shape: pltpu.VMEM(shape, BF16)
    f32 = lambda *shape: pltpu.VMEM(shape, F32)
    s.add("gathered", b16(4, SEQ, H * NOPE))
    s.add("rows", f32(16, GROUP * NOPE))
    s.add("wuk", b16(128, H * NOPE))
    s.add("tall", f32(16, GROUP, NOPE))
    s.add("made", b16(4, SEQ, H, NOPE))
    s.add("queries", b16(SEQ, H, KV_RANK + ROPE))
    s.add("wuv", b16(4, 128, 256))
    s.add("cache", b16(SEQ, KV_RANK + ROPE, CACHE))
    s.add("scores", f32(SEQ, H, CACHE))
    s.add("lanes", f32(KV_RANK // 128, H, 128))
    s.add("mixed", f32(KV_RANK // 128, H // 2, NB, 128))
    s.add("wout", b16(256, D))
    s.add("gates", b16(4, FF_OWN, D))
    s.add("downs", b16(2, FF_OWN, D))
    s.add("sums", f32(4 * FF_OWN, 64 * NB))
    s.add("turned", b16(2 * FF_OWN, 64 * NB))
    s.add("blocks", *[f32(4 * NB, w) for w in WIDTHS])
    s.add("gain", f32(1, D))
    s.add("rope", f32(SEQ, H, 128))
    for f in range(1):
        s.add(f"lat{f}", b16(H // 2, 2, NB, KV_RANK))
        s.add(f"got{f}", b16(H // 2, 2, NB, KV_RANK))
        s.add(f"resid{f}", f32(NB, D))
        for name, shape in (
            ("part2", (4, 4, 2 * NB, HALF)),
            ("next2", (4, 2, NB, HALF)),
            ("land2", (7, NB, HALF)),
            ("land1", (RINGS_PROJECT, 6, 2 * NB, half)),
            ("pass1", (RINGS_PROJECT, 2, 2 * NB, half)),
            ("whole1", (4 - RINGS_PROJECT, 3, 2 * NB, HALF)),
        ):
            s.add(f"{name}{f}", *[b16(*shape)] * 2)
        for name, lead in (
            ("slots", (4, 4, NB)),
            ("all_rows", (4, 4, 4 * NB)),
            ("parts", (4, 4, 4 * NB)),
            ("lasts", (4, 4, NB)),
            ("landings3", (15, NB)),
            ("wholes", (4 - RINGS, 3, 4 * NB)),
        ):
            s.add(f"{name}{f}", *[b16(*lead, w) for w in WIDTHS])
        for name, lead in (
            ("landings", (RINGS, 6, 4 * NB)),
            ("passings", (RINGS, 2, 4 * NB)),
        ):
            s.add(f"{name}{f}", *[b16(*lead, h) for h in halves])
    count = 6 + 6 * (H // GROUP) + 62 + 2 * (24 + 7) + 3 * (15 + 24) * 2
    s.add("local_sems", pltpu.SemaphoreType.DMA((5,)))
    s.add("wuk_sems", pltpu.SemaphoreType.DMA((H // GROUP,)))
    s.add("cache_sems", pltpu.SemaphoreType.DMA((SEQ,)))
    s.add("send_sems", pltpu.SemaphoreType.DMA((count,)))
    s.add("recv_sems", pltpu.SemaphoreType.DMA((count,)))
    return s


def layer_kernel(
    len_ref, q_ref, rope_ref, new_ref, hidden_ref, gain_ref,
    cache_hbm, wuk_hbm, wuv_hbm, wout_hbm, wg_hbm, wu_hbm, wd_hbm, out_ref, *refs,
):
    s = declare().bind(refs)
    at = coordinates()
    r, g = at["r"], at["g"]
    y_lo = g // 16
    copies = Copies(s.send_sems, s.recv_sems)
    every = range(3)

    def peer_along(axis, step):
        return device_at(at, **{axis: (at[axis] + step) % 4})

    def side(axis):
        return at[axis], peer_along(axis, 3), peer_along(axis, 1)

    def three(axis):
        return [peer_along(axis, step) for step in (2, 1, 3)]

    wide = GROUP * NOPE
    spans = [pl.ds(i * wide, wide) for i in range(H // GROUP)]
    wuk_loads = [
        pltpu.make_async_copy(wuk_hbm.at[:, span], s.wuk.at[:, span], s.wuk_sems.at[i])
        for i, span in enumerate(spans)
    ]
    mine = wuv_hbm.at[:, pl.ds(pl.multiple_of(g * 256, 256), 256)]
    own_wuv = pltpu.make_async_copy(mine, s.wuv.at[r], s.local_sems.at[4])
    cache_loads = [
        pltpu.make_async_copy(cache_hbm.at[b], s.cache.at[b], s.cache_sems.at[b]) for b in range(SEQ)
    ]
    loads = [
        pltpu.make_async_copy(src, dst, s.local_sems.at[i])
        for i, (src, dst) in enumerate(
            ((wout_hbm, s.wout), (wg_hbm, s.gates.at[0]), (wu_hbm, s.gates.at[2]), (wd_hbm, s.downs.at[0]))
        )
    ]
    for load in wuk_loads + [own_wuv] + cache_loads + loads:
        load.start()

    twin = (r + 1 - 2 * at["core"], g)
    other = (r + 2) % 4
    cousins = [((r + k) % 4, g) for k in (1, 2, 3)]
    peers = [(r, (g + k) % 32) for k in range(1, 32)]
    across = (r, (g + 16) % 32)
    far_y = [
        device_at(at, **{axis: (at[axis] + k) % 4, "y": 2 * (1 - at["y"] // 2) + j})
        for axis in "xz"
        for k in range(4)
        for j in range(2)
        if axis == "x" or k > 0
    ]
    near_y = [(r + 1 - 2 * at["core"], g), (other + 1 - 2 * at["core"], g)]
    barrier_with(peers + near_y + far_y)

    incoming = [
        [copies.start(q_ref.at[:, span], s.gathered.at[r, :, span], peer) for peer in cousins]
        for span in spans
    ]
    s.gathered[r] = q_ref[...]
    for k in range(H // 2):
        pair = rope_ref[:, pl.ds(k * 128, 128)].astype(F32)
        s.rope[:, 2 * k, :] = pair
        s.rope[:, 2 * k + 1, :] = pltpu.roll(pair, 64, 1)
    s.queries[:, :, pl.ds(KV_RANK, ROPE)] = s.rope[:, :, pl.ds(0, ROPE)].astype(BF16)
    gain = gain_ref[...].astype(F32)
    for k in range(D // 128):
        s.gain[:, pl.ds(k * 128, 128)] = gain[k : k + 1]
    slice_of_rank = pl.ds(pl.multiple_of(r * NOPE, NOPE), NOPE)
    new_rows = new_ref[...].astype(F32)

    def rotary_scores(b):
        length = len_ref[b]
        q = s.rope[b, :, pl.ds(0, ROPE)].astype(BF16)
        lane = iota((H, BLOCK), 1)
        cache_loads[b].wait()
        for c in range(CACHE // BLOCK):
            cols = pl.ds(c * BLOCK, BLOCK)
            v = jnp.dot(q, s.cache[b, pl.ds(KV_RANK, ROPE), cols], preferred_element_type=F32) * SCALE
            s.scores[b, :, cols] = jnp.where(lane < length - c * BLOCK, v, -jnp.inf)

    rotary_scores(0)
    rotary_scores(1)
    back = []
    for i, span in enumerate(spans):
        for copy in incoming[i]:
            copy.wait_recv()
        wuk_loads[i].wait()
        for m in range(4):
            s.rows[pl.ds(4 * m, 4), :] = s.gathered[m, :, span].astype(F32)
        for k in range(GROUP):
            s.tall[:, k, :] = lax.dot_general(
                s.rows[:, pl.ds(k * NOPE, NOPE)].astype(BF16),
                s.wuk[:, pl.ds((i * GROUP + k) * NOPE, NOPE)],
                NT,
                preferred_element_type=F32,
            )
        heads = pl.ds(i * GROUP, GROUP)
        s.made[:, :, heads, :] = s.tall[...].astype(BF16).reshape(4, SEQ, GROUP, NOPE)
        for peer in cousins:
            back.append(
                copies.start(s.made.at[peer[0], :, heads, :], s.queries.at[:, heads, slice_of_rank], peer)
            )
    weights = [copies.start(mine, s.wuv.at[r], peer) for peer in cousins]
    traded = [
        copies.start(src, dst, twin)
        for src, dst in ((wg_hbm, s.gates.at[1]), (wu_hbm, s.gates.at[3]), (wd_hbm, s.downs.at[1]))
    ]
    s.queries[:, :, slice_of_rank] = s.made[r]
    rotary_scores(2)
    rotary_scores(3)
    for copy in back:
        copy.wait_recv()

    def attend(b, local):
        q = s.queries[b]
        new = new_rows[b : b + 1]
        own = jnp.sum(q.astype(F32) * new, axis=1, keepdims=True) * SCALE
        q = q[:, :KV_RANK]
        top = jnp.full((H, 128), -jnp.inf, F32)
        for c in range(CACHE // BLOCK):
            cols = pl.ds(c * BLOCK, BLOCK)
            v = jnp.dot(q, s.cache[b, pl.ds(0, KV_RANK), cols], preferred_element_type=F32) * SCALE
            v += s.scores[b, :, cols]
            s.scores[b, :, cols] = v
            for i in range(BLOCK // 128):
                top = jnp.maximum(top, v[:, i * 128 : (i + 1) * 128])
        top = jnp.maximum(jnp.max(top, axis=1, keepdims=True), own)
        own = jnp.exp(own - top)
        total = jnp.zeros((H, 128), F32)
        mix = own * new[:, :KV_RANK]
        for c in range(CACHE // BLOCK):
            cols = pl.ds(c * BLOCK, BLOCK)
            p = jnp.exp(s.scores[b, :, cols] - top)
            for i in range(BLOCK // 128):
                total += p[:, i * 128 : (i + 1) * 128]
            mix += lax.dot_general(
                p.astype(BF16), s.cache[b, pl.ds(0, KV_RANK), cols], NT, preferred_element_type=F32
            )
        mix = mix / (jnp.sum(total, axis=1, keepdims=True) + own)
        for t in range(KV_RANK // 128):
            s.lanes[t] = mix[:, t * 128 : (t + 1) * 128]
            for h in range(2):
                s.mixed[t, :, 2 * local + h, :] = s.lanes[t, pl.ds(h, H // 2, stride=2), :]

    def place(p, i):
        b = i & (NB - 1)
        of = {"z": (i >> LB) & 3, "y": (i >> (LB + 2)) & 3, "x": (i >> (LB + 4)) & 3}
        t, u, v = (of[axis] for axis in AXES[p])
        return ((t * 4 + u) * 4 + v) * NB + b

    lat, got = s.lat0, s.got0

    def send_latents(pair):
        for t in range(KV_RANK // 128):
            lat[:, pair, :, pl.ds(t * 128, 128)] = s.mixed[t].astype(BF16)
        return [copies.start(lat.at[peer[1], pair], got.at[g, pair], peer) for peer in peers]

    def flow(f):
        buf = lambda name: getattr(s, f"{name}{f}")
        arriving = send_latents(1)
        got[g] = lat[g]
        yield
        for copy in early + arriving:
            copy.wait_recv()
        if f == 0:
            for copy in weights:
                copy.wait_recv()
            own_wuv.wait()
            loads[0].wait()
        rows_in = got[...].reshape(64 * NB, KV_RANK)
        heads = jnp.dot(rows_in, s.wuv[...].reshape(KV_RANK, 256), preferred_element_type=F32)
        row, col = iota((64 * NB, 256), 0), iota((64 * NB, 256), 1)
        heads = jnp.where((row & 1) == (col >> 7), heads, 0.0).astype(BF16)
        row, col = iota((32 * NB, 64 * NB), 0), iota((32 * NB, 64 * NB), 1)
        b, y_of, low, high = row & (NB - 1), (row >> LB) & 1, (row >> (LB + 1)) & 3, row >> (LB + 3)
        part2, next2, land2 = buf("part2"), buf("next2"), buf("land2")
        rings = [[], []]
        gathering = [[], []]

        def project(x_of, z_of, part, first_col):
            source = (((y_of * 4 + x_of) * 4) + z_of) * NB + b
            pick = jnp.where((col >> 1) == source, 1.0, 0.0).astype(BF16)
            rows = jnp.dot(pick, heads, preferred_element_type=F32).astype(BF16)
            step = HALF // 4
            for n in range(4):
                out = jnp.dot(
                    rows, s.wout[:, pl.ds(first_col + n * step, step)], preferred_element_type=F32
                )
                part[:, :, :, pl.ds(n * step, step)] = out.reshape(4, 4, 2 * NB, step).astype(BF16)

        def start2(i, k):
            j = (at[AXES2[i][1]] + STEPS[k]) % 4
            first = AXES2[i][0]
            chunk = lambda t, cut: part2[i].at[t, j, :, pl.ds(*cut)]
            if k in DIRECT_PROJECT:
                ring = ScatterDirect(copies, chunk, buf("whole1")[i].at[k - RINGS_PROJECT], at[first], three(first), HALF_CUT)
            else:
                ring = ScatterRing(
                    copies, chunk, buf("land1")[i].at[k], buf("pass1")[i].at[k], side(first), HALF_CUT
                )
            ring.start()
            rings[i].append(ring)

        def end2(i, k):
            second = AXES2[i][1]
            j = (at[second] + STEPS[k]) % 4
            for cut, value in zip(HALF_CUT, rings[i][k].end()):
                for half in range(2):
                    next2[i][j, half, :, pl.ds(*cut)] = value[NB * half : NB * half + NB].astype(BF16)
            for step in (1, 0):
                if k < 3 or step > 0:
                    to = (y_lo + step) % 2
                    device = device_at(at, **{second: j, "y": at["y"] - y_lo + to})
                    landing = land2[i].at[len(gathering[i])]
                    gathering[i].append(copies.start(next2[i].at[j, to], landing, device))

        project(high, low, part2[0], 0)
        start2(0, 0)
        start2(0, 1)
        project(low, high, part2[1], HALF)
        start2(1, 0)
        start2(1, 1)
        for k in range(4):
            yield
            for i in range(2):
                rings[i][k].middle()
                if k < 2:
                    start2(i, k + 2)
            if k >= LAG:
                for i in range(2):
                    end2(i, k - LAG)
        for k in range(4 - LAG, 4):
            yield
            for i in range(2):
                end2(i, k)
        yield
        squares = jnp.zeros((NB, 1), F32)
        kept = []
        for i in range(2):
            cols = pl.ds(i * HALF, HALF)
            total = next2[i][at[AXES2[i][1]], y_lo].astype(F32) + hidden_ref[:, cols].astype(F32)
            for k in range(7):
                gathering[i][k].wait_recv()
                total += land2[i][k].astype(F32)
            resid = total.astype(BF16).astype(F32)
            buf("resid")[:, cols] = resid
            kept.append(resid)
            squares += jnp.sum(resid * resid, axis=1, keepdims=True)
        factor = lax.rsqrt(squares / D + EPS)
        normed = jnp.concatenate(kept, axis=1) * factor * s.gain[...]
        normed = normed.astype(BF16)

        slots, all_rows = buf("slots"), buf("all_rows")
        plane = [{}, {}, {}]
        for p in every:
            _, second, last = AXES[p]
            slots[p][at[second], at[last]] = normed[:, STARTS[p] : STARTS[p] + WIDTHS[p]]
        for step in (0, 1, 3, 2):
            for p in every:
                _, second, last = AXES[p]
                block = slots[p].at[at[second], at[last]]
                plane[p][step] = [
                    copies.start(
                        block,
                        block,
                        device_at(at, **{second: (at[second] + step) % 4, last: (at[last] + k) % 4}),
                    )
                    for k in (2, 1, 3, 0)
                    if step > 0 or k > 0
                ]
        yield
        third = [{}, {}, {}]

        def start3(p, step):
            first, second, _ = AXES[p]
            j = (at[second] + step) % 4
            for copy in plane[p][(4 - step) % 4]:
                copy.wait_recv()
            for m in range(4):
                s.blocks[p][pl.ds(NB * m, NB), :] = slots[p][j, m].astype(F32)
            all_rows[p][at[first], j] = s.blocks[p][...].astype(BF16)
            if step in DIRECT_GATHER:
                ring = GatherDirect(copies, lambda t: all_rows[p].at[t, j], at[first], three(first))
            else:
                ring = GatherRing(
                    copies, lambda t, cut: all_rows[p].at[t, j, :, pl.ds(*cut)], side(first), CUTS[p]
                )
            ring.start()
            third[p][step] = ring

        for step in (0, 3, 1, 2):
            for p in every:
                start3(p, step)
            if step == 1:
                for p in every:
                    third[p][0].middle()
        for step in (3, 1, 2):
            for p in every:
                third[p][step].middle()
        yield
        if f == 0:
            for load in loads[1:]:
                load.wait()
            for copy in traded:
                copy.wait_recv()
        row, col = iota((64 * NB, 64 * NB), 0), iota((64 * NB, 64 * NB), 1)
        for p in every:
            for step in (0, 3, 1, 2):
                third[p][step].near()
                third[p][step].far()
            rows = all_rows[p][...].reshape(64 * NB, WIDTHS[p])
            if p > 0:
                order = jnp.where(col == place(p, row), 1.0, 0.0).astype(BF16)
                rows = jnp.dot(order, rows, preferred_element_type=F32).astype(BF16)
            matrix = s.gates[:, :, pl.ds(STARTS[p], WIDTHS[p])].reshape(4 * FF_OWN, WIDTHS[p])
            product = lax.dot_general(matrix, rows, NT, preferred_element_type=F32)
            if p > 0:
                product += s.sums[...]
            s.sums[...] = product
        gate, up = s.sums[pl.ds(0, 2 * FF_OWN), :], s.sums[pl.ds(2 * FF_OWN, 2 * FF_OWN), :]
        s.turned[...] = (gate / (1.0 + jnp.exp(-gate)) * up).astype(BF16)

        parts, lasts = buf("parts"), buf("lasts")
        first = [[], [], []]

        def start1(p, k):
            j = (at[AXES[p][1]] + STEPS[k]) % 4
            axis = AXES[p][0]
            chunk = lambda t, cut: parts[p].at[k, t, :, pl.ds(*cut)]
            if k in DIRECT_SCATTER:
                ring = ScatterDirect(copies, chunk, buf("wholes")[p].at[k - RINGS], at[axis], three(axis), CUTS[p])
            else:
                ring = ScatterRing(
                    copies, chunk, buf("landings")[p].at[k], buf("passings")[p].at[k], side(axis), CUTS[p]
                )
            ring.start()
            first[p].append(ring)

        ending = [[], [], []]

        def end1(p, k):
            _, second, last = AXES[p]
            j = (at[second] + STEPS[k]) % 4
            for (start, size), value in zip(CUTS[p], first[p][k].end()):
                for m in range(4):
                    lasts[p][j, m, :, pl.ds(start, size)] = value[NB * m : NB * m + NB].astype(BF16)
            for step in (2, 1, 3, 0):
                if k < 3 or step > 0:
                    to = (at[last] + step) % 4
                    device = device_at(at, **{second: j, last: to})
                    landing = buf("landings3")[p].at[len(ending[p])]
                    ending[p].append(copies.start(lasts[p].at[j, to], landing, device))

        acts = []
        for p in every:
            k = row >> (LB + 4)
            step = jnp.where(k == 0, 2, jnp.where(k == 1, 1, jnp.where(k == 2, 3, 0)))
            lead = (row >> (LB + 2)) & 3
            middle = (step + at[AXES[p][1]]) & 3
            index = (lead * 4 + middle) * (4 * NB) + (row & (4 * NB - 1))
            order = jnp.where(index == place(p, col), 1.0, 0.0).astype(BF16)
            acts.append(lax.dot_general(order, s.turned[...], NT, preferred_element_type=F32).astype(BF16))
        for k in (0, 2):
            for p in every:
                for start, size in CUTS[p]:
                    matrix = s.downs[:, :, pl.ds(STARTS[p] + start, size)].reshape(2 * FF_OWN, size)
                    out = jnp.dot(
                        acts[p][16 * NB * k : 16 * NB * (k + 2)], matrix, preferred_element_type=F32
                    )
                    out = out.reshape(2, 4, 4 * NB, size).astype(BF16)
                    parts[p][pl.ds(k, 2), :, :, pl.ds(start, size)] = out
                for one in (k, k + 1):
                    if one < START_AHEAD:
                        start1(p, one)
        for k in range(4):
            yield
            for p in every:
                first[p][k].middle()
                if k + START_AHEAD < 4:
                    start1(p, k + START_AHEAD)
            if k >= LAG:
                for p in every:
                    end1(p, k - LAG)
        for k in range(4 - LAG, 4):
            yield
            for p in every:
                end1(p, k)
        yield
        for p in every:
            _, second, last = AXES[p]
            cols = pl.ds(STARTS[p], WIDTHS[p])
            total = buf("resid")[:, cols] + lasts[p][at[second], at[last]].astype(F32)
            for k in range(15):
                ending[p][k].wait_recv()
                total += buf("landings3")[p][k].astype(F32)
            out_ref[:, cols] = total.astype(BF16)
        yield

    early = []
    for b in range(SEQ):
        attend(b, b % 2)
        if b == 1:
            early = send_latents(0)
    for _ in flow(0):
        pass
    copies.finish()


def on_device(
    hidden_in, q_nope, q_rope, new_kv, cache_kv, lengths,
    w_uk, w_uv, w_out, norm_gain, w_gate, w_up, w_down,
):
    vmem = pl.BlockSpec(memory_space=pltpu.VMEM)
    hbm = pl.BlockSpec(memory_space=pl.ANY)
    return pl.pallas_call(
        layer_kernel,
        out_shape=jax.ShapeDtypeStruct((SEQ, D), BF16),
        in_specs=[pl.BlockSpec(memory_space=pltpu.SMEM)] + [vmem] * 5 + [hbm] * 7,
        out_specs=vmem,
        scratch_shapes=declare().shapes,
        compiler_params=pltpu.CompilerParams(
            collective_id=0, has_side_effects=True, vmem_limit_bytes=VMEM_LIMIT
        ),
        name="layer",
    )(
        lengths, q_nope, q_rope, new_kv, hidden_in, norm_gain.reshape(D // 128, 128),
        jnp.swapaxes(cache_kv, 1, 2), w_uk, w_uv, w_out, w_gate.T, w_up.T, w_down,
    )


def solution(mesh):
    return jax.shard_map(
        on_device,
        mesh=mesh,
        in_specs=(
            P(("rep", "grp"), None),
            P(("rep", "grp"), None),
            P(("rep", "grp"), None),
            P(("rep", "grp"), None),
            P(("rep", "grp"), None, None),
            P(("rep", "grp")),
            P("rep", None),
            P("rep", None),
            P("grp", None),
            P(),
            P(None, ("rep", "grp")),
            P(None, ("rep", "grp")),
            P(("rep", "grp"), None),
        ),
        out_specs=P(("rep", "grp"), None),
        check_vma=False,
    )
```
